32 devices in a mesh: dp: 4 (over y, core), ctx: 4 (over z), tp: 2 (over x).
Axes of the slice: x: 2, y: 2, z: 4, core: 2. Of those that a mesh axis runs over, the one named last changes fastest.
Arguments:
- img_in: bfloat16 [4, 512, 1536], P('dp', 'ctx'), may hold values from -6 to 6
- txt_in: bfloat16 [4, 154, 1536], P('dp'), may hold values from -6 to 6
- cond: bfloat16 [4, 1536], P(None, ('dp', 'ctx', 'tp')), may hold values from -6 to 6
- mod_weight: float32 [1, 2, 1536, 6, 1536], P(None, None, ('dp', 'ctx', 'tp')), may hold values from -0.15625 to 0.15625
- qkv_weight: float32 [1, 2, 1536, 3, 1536], P(None, None, ('dp', 'ctx'), None, 'tp'), may hold values from -0.15625 to 0.15625
- out_weight: float32 [1, 2, 1536, 1536], P(None, None, 'tp', ('dp', 'ctx')), may hold values from -0.75 to 0.75
- up_weight: float32 [1, 2, 1536, 6144], P(None, None, ('dp', 'ctx'), 'tp'), may hold values from -0.15625 to 0.15625
- down_weight: float32 [1, 2, 6144, 1536], P(None, None, 'tp', ('dp', 'ctx')), may hold values from -0.078125 to 0.078125
- norm_gain: float32 [1, 2, 2, 64], replicated, may hold values from 0.7 to 1.8
- cot_img: bfloat16 [4, 512, 1536], P('dp', 'ctx'), may hold values from -6 to 6
- cot_txt: bfloat16 [4, 154, 1536], P('dp'), may hold values from -6 to 6
- mod_moment: float32 [1, 2, 1536, 6, 1536], P(None, None, ('dp', 'ctx', 'tp')), may hold values from -6 to 6
- qkv_moment: float32 [1, 2, 1536, 3, 1536], P(None, None, ('dp', 'ctx'), None, 'tp'), may hold values from -6 to 6
- out_moment: float32 [1, 2, 1536, 1536], P(None, None, 'tp', ('dp', 'ctx')), may hold values from -6 to 6
- up_moment: float32 [1, 2, 1536, 6144], P(None, None, ('dp', 'ctx'), 'tp'), may hold values from -6 to 6
- down_moment: float32 [1, 2, 6144, 1536], P(None, None, 'tp', ('dp', 'ctx')), may hold values from -6 to 6
- gain_moment: float32 [1, 2, 2, 64], replicated, may hold values from -6 to 6
- mod_second: float32 [1, 2, 1536, 6, 1536], P(None, None, ('dp', 'ctx', 'tp')), may hold values from 0.5 to 2
- qkv_second: float32 [1, 2, 1536, 3, 1536], P(None, None, ('dp', 'ctx'), None, 'tp'), may hold values from 0.5 to 2
- out_second: float32 [1, 2, 1536, 1536], P(None, None, 'tp', ('dp', 'ctx')), may hold values from 0.5 to 2
- up_second: float32 [1, 2, 1536, 6144], P(None, None, ('dp', 'ctx'), 'tp'), may hold values from 0.5 to 2
- down_second: float32 [1, 2, 6144, 1536], P(None, None, 'tp', ('dp', 'ctx')), may hold values from 0.5 to 2
- gain_second: float32 [1, 2, 2, 64], replicated, may hold values from 0.5 to 2
Outputs:
- img_out: bfloat16 [4, 512, 1536], P('dp', 'ctx')
- txt_out: bfloat16 [4, 154, 1536], P('dp')
- img_grad: bfloat16 [4, 512, 1536], P('dp', 'ctx')
- txt_grad: bfloat16 [4, 154, 1536], P('dp')
- mod_grad: float32 [1, 2, 1536, 6, 1536], P(None, None, ('dp', 'ctx', 'tp'))
- mod_next: float32 [1, 2, 1536, 6, 1536], P(None, None, ('dp', 'ctx', 'tp'))
- mod_moment_next: float32 [1, 2, 1536, 6, 1536], P(None, None, ('dp', 'ctx', 'tp'))
- mod_second_next: float32 [1, 2, 1536, 6, 1536], P(None, None, ('dp', 'ctx', 'tp'))
- qkv_grad: float32 [1, 2, 1536, 3, 1536], P(None, None, ('dp', 'ctx'), None, 'tp')
- qkv_next: float32 [1, 2, 1536, 3, 1536], P(None, None, ('dp', 'ctx'), None, 'tp')
- qkv_moment_next: float32 [1, 2, 1536, 3, 1536], P(None, None, ('dp', 'ctx'), None, 'tp')
- qkv_second_next: float32 [1, 2, 1536, 3, 1536], P(None, None, ('dp', 'ctx'), None, 'tp')
- out_grad: float32 [1, 2, 1536, 1536], P(None, None, 'tp', ('dp', 'ctx'))
- out_next: float32 [1, 2, 1536, 1536], P(None, None, 'tp', ('dp', 'ctx'))
- out_moment_next: float32 [1, 2, 1536, 1536], P(None, None, 'tp', ('dp', 'ctx'))
- out_second_next: float32 [1, 2, 1536, 1536], P(None, None, 'tp', ('dp', 'ctx'))
- up_grad: float32 [1, 2, 1536, 6144], P(None, None, ('dp', 'ctx'), 'tp')
- up_next: float32 [1, 2, 1536, 6144], P(None, None, ('dp', 'ctx'), 'tp')
- up_moment_next: float32 [1, 2, 1536, 6144], P(None, None, ('dp', 'ctx'), 'tp')
- up_second_next: float32 [1, 2, 1536, 6144], P(None, None, ('dp', 'ctx'), 'tp')
- down_grad: float32 [1, 2, 6144, 1536], P(None, None, 'tp', ('dp', 'ctx'))
- down_next: float32 [1, 2, 6144, 1536], P(None, None, 'tp', ('dp', 'ctx'))
- down_moment_next: float32 [1, 2, 6144, 1536], P(None, None, 'tp', ('dp', 'ctx'))
- down_second_next: float32 [1, 2, 6144, 1536], P(None, None, 'tp', ('dp', 'ctx'))
- gain_grad: float32 [1, 2, 2, 64], replicated
- gain_next: float32 [1, 2, 2, 64], replicated
- gain_moment_next: float32 [1, 2, 2, 64], replicated
- gain_second_next: float32 [1, 2, 2, 64], replicated
The draws below stay inside these ranges and needn't reach their ends.
All inputs are finite; a program needn't handle non-finite values.
Results may differ from the reference program's by a relative error of at most 0.025.
Values may be sent and summed in bfloat16 or wider, within the bound.
A program may use at most 320 MiB of HBM per device.

```python
import math
import jax
import jax.numpy as jnp
from jax import lax

D = 1536
HD = 64
FF = 6144
IMG = 512
TXT = 154
LAYERS = 1
SEQS = 4
N_TP = 2


def draw_norm_gain(key, part):
    return jax.random.uniform(key, (LAYERS, 2, 2, HD), jnp.float32, 0.7, 1.5)


def steps_of(key, dims, pieces, smallest, largest):
    def one(position, shards_of):
        heights = jax.random.uniform(jax.random.fold_in(jax.random.fold_in(key, 6), position), (shards_of,), jnp.float32, smallest / len(pieces), largest / len(pieces))
        return jnp.repeat(jnp.exp(heights), dims[position] // shards_of).reshape((-1,) + (1,) * (len(dims) - position - 1))

    gain = one(*pieces[0])
    for cut in pieces[1:]:
        gain = gain * one(*cut)
    return gain


def normal_values(rng, extent, deviation, limit, pieces=(), held_as=jnp.bfloat16):
    drawn = deviation * jax.random.normal(rng, extent, jnp.float32)
    if pieces:
        drawn = drawn * steps_of(rng, extent, pieces, -0.22, 0.18)
    return jnp.clip(drawn, -limit, limit).astype(held_as)


def setup_inputs(seed: int = 0) -> dict:
    splits = jax.random.split(jax.random.key(seed), 24)
    img_in = normal_values(splits[0], (SEQS, IMG, D), 1.0, 6.0, ((0, 4), (1, 4)))
    txt_in = normal_values(splits[1], (SEQS, TXT, D), 1.0, 6.0, ((0, 4),))
    cond = normal_values(splits[2], (SEQS, D), 1.0, 6.0, ((1, 32),))
    mod_weight = normal_values(splits[3], (LAYERS, 2, D, 6, D), D ** -0.5, 0.15625, ((2, 32),), jnp.float32)
    qkv_weight = normal_values(splits[4], (LAYERS, 2, D, 3, D), D ** -0.5, 0.15625, ((2, 16), (4, 2)), jnp.float32)
    out_weight = normal_values(splits[5], (LAYERS, 2, D, D), HD ** -0.5, 0.75, ((2, 2), (3, 16)), jnp.float32)
    up_weight = normal_values(splits[6], (LAYERS, 2, D, FF), D ** -0.5, 0.15625, ((2, 16), (3, 2)), jnp.float32)
    down_weight = normal_values(splits[7], (LAYERS, 2, FF, D), FF ** -0.5, 0.078125, ((2, 2), (3, 16)), jnp.float32)
    norm_gain = draw_norm_gain(jax.random.fold_in(splits[23], 71), 0)
    cot_img = normal_values(splits[9], (SEQS, IMG, D), 1.0, 6.0, ((0, 4), (1, 4)))
    cot_txt = normal_values(splits[10], (SEQS, TXT, D), 1.0, 6.0, ((0, 4),))
    mod_moment = normal_values(splits[11], (LAYERS, 2, D, 6, D), 1.0, 6.0, ((2, 32),), jnp.float32)
    qkv_moment = normal_values(splits[12], (LAYERS, 2, D, 3, D), 1.0, 6.0, ((2, 16), (4, 2)), jnp.float32)
    out_moment = normal_values(splits[13], (LAYERS, 2, D, D), 1.0, 6.0, ((2, 2), (3, 16)), jnp.float32)
    up_moment = normal_values(splits[14], (LAYERS, 2, D, FF), 1.0, 6.0, ((2, 16), (3, 2)), jnp.float32)
    down_moment = normal_values(splits[15], (LAYERS, 2, FF, D), 1.0, 6.0, ((2, 2), (3, 16)), jnp.float32)
    gain_moment = normal_values(splits[16], (LAYERS, 2, 2, HD), 1.0, 6.0, (), jnp.float32)
    mod_second = jnp.clip(jnp.exp(math.log(2.0) - 1.3862944 * jax.random.uniform(splits[17], (LAYERS, 2, D, 6, D), jnp.float32) ** steps_of(splits[17], (LAYERS, 2, D, 6, D), ((2, 32),), -0.2, 0.2)), 0.5, 2.0)
    qkv_second = jnp.clip(jnp.exp(math.log(2.0) - 1.3862944 * jax.random.uniform(splits[18], (LAYERS, 2, D, 3, D), jnp.float32) ** steps_of(splits[18], (LAYERS, 2, D, 3, D), ((2, 16), (4, 2)), -0.2, 0.2)), 0.5, 2.0)
    out_second = jnp.clip(jnp.exp(math.log(2.0) - 1.3862944 * jax.random.uniform(splits[19], (LAYERS, 2, D, D), jnp.float32) ** steps_of(splits[19], (LAYERS, 2, D, D), ((2, 2), (3, 16)), -0.2, 0.2)), 0.5, 2.0)
    up_second = jnp.clip(jnp.exp(math.log(2.0) - 1.3862944 * jax.random.uniform(splits[20], (LAYERS, 2, D, FF), jnp.float32) ** steps_of(splits[20], (LAYERS, 2, D, FF), ((2, 16), (3, 2)), -0.2, 0.2)), 0.5, 2.0)
    down_second = jnp.clip(jnp.exp(math.log(2.0) - 1.3862944 * jax.random.uniform(splits[21], (LAYERS, 2, FF, D), jnp.float32) ** steps_of(splits[21], (LAYERS, 2, FF, D), ((2, 2), (3, 16)), -0.2, 0.2)), 0.5, 2.0)
    gain_second = jnp.clip(jnp.exp(jax.random.uniform(splits[22], (LAYERS, 2, 2, HD), jnp.float32, math.log(0.5), math.log(2.0))), 0.5, 2.0)
    return {"img_in": img_in, "txt_in": txt_in, "cond": cond, "mod_weight": mod_weight, "qkv_weight": qkv_weight, "out_weight": out_weight, "up_weight": up_weight, "down_weight": down_weight, "norm_gain": norm_gain, "cot_img": cot_img, "cot_txt": cot_txt, "mod_moment": mod_moment, "qkv_moment": qkv_moment, "out_moment": out_moment, "up_moment": up_moment, "down_moment": down_moment, "gain_moment": gain_moment, "mod_second": mod_second, "qkv_second": qkv_second, "out_second": out_second, "up_second": up_second, "down_second": down_second, "gain_second": gain_second}


norm_eps = 1e-06
learn_rate = 0.004
beta_one = 0.9
beta_two = 0.999
adam_eps = 1e-08
decay_rate = 0.1
corr_one = 1.0 - beta_one ** 3
corr_two = 1.0 - beta_two ** 3

def product(pattern, former, latter):
    return jnp.einsum(pattern, former.astype(jnp.float32), latter.astype(jnp.float32), precision=lax.Precision.HIGHEST)

def layer_norm(values):
    center = values - lax.optimization_barrier(jnp.mean(values, axis=-1, keepdims=True))
    spread = lax.rsqrt(lax.optimization_barrier(jnp.mean(center * center, axis=-1, keepdims=True)) + norm_eps)
    return (center * spread, spread)

def norm_back(incoming, normed, spread):
    return spread * (incoming - lax.optimization_barrier(jnp.mean(incoming, axis=-1, keepdims=True)) - normed * lax.optimization_barrier(jnp.mean(incoming * normed, axis=-1, keepdims=True)))

def rms_norm(raw_rows):
    factor = lax.rsqrt(lax.optimization_barrier(jnp.mean(raw_rows * raw_rows, axis=-1, keepdims=True)) + norm_eps)
    return (raw_rows * factor, factor)

def rms_back(incoming, normed, factor):
    return factor * (incoming - normed * lax.optimization_barrier(jnp.mean(incoming * normed, axis=-1, keepdims=True)))

def gelu_tanh(values):
    return jax.nn.gelu(values, approximate=True)

def adam_step(weight, moment, second, gradient):
    new_moment = beta_one * moment + (1.0 - beta_one) * gradient
    new_second = beta_two * second + (1.0 - beta_two) * gradient * gradient
    update = new_moment / corr_one / (jnp.sqrt(new_second / corr_two) + adam_eps) + decay_rate * weight
    return (weight - learn_rate * update, new_moment, new_second)

def modulate(normed, shift_vec, scale_vec):
    return (normed * (1.0 + scale_vec[:, None, :]) + shift_vec[:, None, :]).astype(jnp.bfloat16)

def stream_front(inputs, modulation, qkv_part, gain_pair):
    values = inputs.astype(jnp.float32)
    normed, spread = layer_norm(values)
    hidden = modulate(normed, modulation[:, 0], modulation[:, 1])
    packed = product('btd,dkc->btkc', hidden, qkv_part)
    packed = packed.reshape(packed.shape[0], packed.shape[1], 3, -1, gain_pair.shape[-1])
    q_hat, q_factor = rms_norm(packed[:, :, 0])
    k_hat, k_factor = rms_norm(packed[:, :, 1])
    return {'values': values, 'normed': normed, 'spread': spread, 'hidden': hidden, 'q_hat': q_hat, 'q_factor': q_factor, 'k_hat': k_hat, 'k_factor': k_factor, 'queries': (q_hat * gain_pair[0]).astype(jnp.bfloat16), 'key_rows': (k_hat * gain_pair[1]).astype(jnp.bfloat16), 'value_rows': packed[:, :, 2].astype(jnp.bfloat16)}

def mlp_front(resid, modulation, up_part):
    normed, spread = layer_norm(resid)
    hidden = modulate(normed, modulation[:, 3], modulation[:, 4])
    pre_act = product('btd,df->btf', hidden, up_part)
    activated = gelu_tanh(pre_act).astype(jnp.bfloat16)
    return {'normed': normed, 'spread': spread, 'hidden': hidden, 'pre_act': pre_act, 'activated': activated}

def attend(query_all, key_all, value_all, scale_factor):
    scores = product('bqhd,bkhd->bhqk', query_all, key_all) * scale_factor
    row_peak = lax.optimization_barrier(jnp.max(scores, axis=-1, keepdims=True))
    log_total = row_peak + jnp.log(lax.optimization_barrier(jnp.sum(jnp.exp(scores - row_peak), axis=-1, keepdims=True)))
    attn_probs = jnp.exp(scores - log_total).astype(jnp.bfloat16)
    attended = product('bhqk,bkhd->bqhd', attn_probs, value_all)
    return (attended, log_total)

def attend_back(grad_att, query_all, key_all, value_all, attended, log_total, scale_factor, split_at):
    row_delta = lax.optimization_barrier(jnp.sum(grad_att.astype(jnp.float32) * attended, axis=-1))
    scores = product('bqhd,bkhd->bhqk', query_all, key_all) * scale_factor
    attn_probs = jnp.exp(scores - log_total)
    prob_grad = product('bqhd,bkhd->bhqk', grad_att, value_all)
    score_grad = (attn_probs * (prob_grad - jnp.transpose(row_delta, (0, 2, 1))[..., None]) * scale_factor).astype(jnp.bfloat16)
    probs_low = attn_probs.astype(jnp.bfloat16)
    query_grad = product('bhqk,bkhd->bqhd', score_grad, key_all)
    key_first = product('bhqk,bqhd->bkhd', score_grad[:, :, :split_at], query_all[:, :split_at])
    key_second = product('bhqk,bqhd->bkhd', score_grad[:, :, split_at:], query_all[:, split_at:])
    value_first = product('bhqk,bqhd->bkhd', probs_low[:, :, :split_at], grad_att[:, :split_at])
    value_second = product('bhqk,bqhd->bkhd', probs_low[:, :, split_at:], grad_att[:, split_at:])
    return (query_grad, key_first, key_second, value_first, value_second)

def mlp_back(grad_out, modulation, mlp_parts, down_out, up_part, down_part):
    gate_two = lax.optimization_barrier(jnp.sum(grad_out * down_out, axis=1))
    branch = (grad_out * modulation[:, 5][:, None, :]).astype(jnp.bfloat16)
    act_grad = product('btd,fd->btf', branch, down_part)
    down_term = product('btf,btd->fd', mlp_parts['activated'], branch)
    pre_grad = jax.vjp(gelu_tanh, mlp_parts['pre_act'])[1](act_grad)[0].astype(jnp.bfloat16)
    up_term = product('btd,btf->df', mlp_parts['hidden'], pre_grad)
    hidden_part = product('btf,df->btd', pre_grad, up_part)
    return (gate_two, down_term, up_term, hidden_part)

def norm_branch_back(hidden_grad, normed, spread, scale_vec, residual_grad):
    shift_grad = lax.optimization_barrier(jnp.sum(hidden_grad, axis=1))
    scale_grad = lax.optimization_barrier(jnp.sum(hidden_grad * normed, axis=1))
    total = residual_grad + norm_back(hidden_grad * (1.0 + scale_vec[:, None, :]), normed, spread)
    return (shift_grad, scale_grad, total)

def attention_branch_back(resid_grad, modulation, proj, flat_rows, out_part):
    gate_one = lax.optimization_barrier(jnp.sum(resid_grad * proj, axis=1))
    branch = (resid_grad * modulation[:, 2][:, None, :]).astype(jnp.bfloat16)
    att_grad = product('btd,cd->btc', branch, out_part)
    out_term = product('btc,btd->cd', flat_rows, branch)
    return (gate_one, att_grad, out_term)

def head_back(query_grad, key_grad, value_grad, front, gain_pair):
    gain_term = jnp.stack([lax.optimization_barrier(jnp.sum(query_grad * front['q_hat'], axis=(0, 1, 2))), lax.optimization_barrier(jnp.sum(key_grad * front['k_hat'], axis=(0, 1, 2)))])
    q_raw = rms_back(query_grad * gain_pair[0], front['q_hat'], front['q_factor'])
    k_raw = rms_back(key_grad * gain_pair[1], front['k_hat'], front['k_factor'])
    packed = jnp.stack([q_raw, k_raw, value_grad], axis=2)
    packed = packed.reshape(packed.shape[0], packed.shape[1], 3, -1).astype(jnp.bfloat16)
    return (gain_term, packed)

def grouped_sum(flat_rows, weight):
    flat_groups = flat_rows.reshape(flat_rows.shape[0], flat_rows.shape[1], N_TP, -1)
    weight_groups = weight.reshape(N_TP, -1, weight.shape[-1])
    partial_terms = product('btgc,gcd->btgd', flat_groups, weight_groups).astype(jnp.bfloat16)
    return lax.optimization_barrier(jnp.sum(partial_terms.astype(jnp.float32), axis=2))

def reference(img_in, txt_in, cond, mod_weight, qkv_weight, out_weight, up_weight, down_weight, norm_gain, cot_img, cot_txt, mod_moment, qkv_moment, out_moment, up_moment, down_moment, gain_moment, mod_second, qkv_second, out_second, up_second, down_second, gain_second):
    scale_factor = HD ** (-0.5)
    cond_act = jax.nn.silu(cond.astype(jnp.float32)).astype(jnp.bfloat16)
    all_mod = product('sm,ltmkc->ltskc', cond_act, mod_weight.astype(jnp.bfloat16))
    seq_mod = jnp.moveaxis(all_mod, 2, 0)
    qkv_low = qkv_weight.astype(jnp.bfloat16)
    out_low = out_weight.astype(jnp.bfloat16)
    up_low = up_weight.astype(jnp.bfloat16)
    down_low = down_weight.astype(jnp.bfloat16)

    def one_sequence(carry, packet):
        qkv_acc, out_acc, up_acc, down_acc, gain_acc = carry
        img_rows, txt_rows, img_cot, txt_cot, modulation = packet
        streams = [img_rows[None].astype(jnp.float32), txt_rows[None].astype(jnp.float32)]
        stored = []
        for layer_id in range(LAYERS):
            mod_pair = [modulation[layer_id, 0][None], modulation[layer_id, 1][None]]
            front_pair = [stream_front(streams[stream_id], mod_pair[stream_id], qkv_low[layer_id, stream_id], norm_gain[layer_id, stream_id]) for stream_id in range(2)]
            key_all = jnp.concatenate([front_pair[0]['key_rows'], front_pair[1]['key_rows']], axis=1)
            value_all = jnp.concatenate([front_pair[0]['value_rows'], front_pair[1]['value_rows']], axis=1)
            query_all = jnp.concatenate([front_pair[0]['queries'], front_pair[1]['queries']], axis=1)
            attended, log_total = attend(query_all, key_all, value_all, scale_factor)
            attended_low = attended.astype(jnp.bfloat16)
            flat_pair = [attended_low[:, :IMG].reshape(1, IMG, -1), attended_low[:, IMG:].reshape(1, TXT, -1)]
            proj_pair = [grouped_sum(flat_pair[stream_id], out_low[layer_id, stream_id]) for stream_id in range(2)]
            resid_pair = [front_pair[stream_id]['values'] + mod_pair[stream_id][:, 2][:, None, :] * proj_pair[stream_id] for stream_id in range(2)]
            mlp_pair = [mlp_front(resid_pair[stream_id], mod_pair[stream_id], up_low[layer_id, stream_id]) for stream_id in range(2)]
            down_pair = [grouped_sum(mlp_pair[stream_id]['activated'], down_low[layer_id, stream_id]) for stream_id in range(2)]
            streams = [resid_pair[stream_id] + mod_pair[stream_id][:, 5][:, None, :] * down_pair[stream_id] for stream_id in range(2)]
            stored.append({'front': front_pair, 'key_all': key_all, 'value_all': value_all, 'query_all': query_all, 'attended': attended, 'log_total': log_total, 'flat': flat_pair, 'proj': proj_pair, 'mlp': mlp_pair, 'down': down_pair})
        grads = [img_cot[None].astype(jnp.float32), txt_cot[None].astype(jnp.float32)]
        mod_list = [None] * LAYERS
        for layer_id in reversed(range(LAYERS)):
            saved = stored[layer_id]
            mod_pair = [modulation[layer_id, 0][None], modulation[layer_id, 1][None]]
            front_pair = saved['front']
            mlp_parts = [mlp_back(grads[stream_id], mod_pair[stream_id], saved['mlp'][stream_id], saved['down'][stream_id], up_low[layer_id, stream_id], down_low[layer_id, stream_id]) for stream_id in range(2)]
            mlp_norm = [norm_branch_back(mlp_parts[stream_id][3], saved['mlp'][stream_id]['normed'], saved['mlp'][stream_id]['spread'], mod_pair[stream_id][:, 4], grads[stream_id]) for stream_id in range(2)]
            attn_parts = [attention_branch_back(mlp_norm[stream_id][2], mod_pair[stream_id], saved['proj'][stream_id], saved['flat'][stream_id], out_low[layer_id, stream_id]) for stream_id in range(2)]
            grad_att = jnp.concatenate([attn_parts[0][1].reshape(1, IMG, -1, HD), attn_parts[1][1].reshape(1, TXT, -1, HD)], axis=1).astype(jnp.bfloat16)
            query_grad, key_first, key_second, value_first, value_second = attend_back(grad_att, saved['query_all'], saved['key_all'], saved['value_all'], saved['attended'], saved['log_total'], scale_factor, IMG)
            key_grad = key_first + key_second
            value_grad = value_first + value_second
            key_pair = [key_grad[:, :IMG], key_grad[:, IMG:]]
            value_pair = [value_grad[:, :IMG], value_grad[:, IMG:]]
            query_pair = [query_grad[:, :IMG], query_grad[:, IMG:]]
            head_parts = [head_back(query_pair[stream_id], key_pair[stream_id], value_pair[stream_id], front_pair[stream_id], norm_gain[layer_id, stream_id]) for stream_id in range(2)]
            input_pair = [product('btkc,dkc->btd', head_parts[stream_id][1], qkv_low[layer_id, stream_id]) for stream_id in range(2)]
            attn_norm = [norm_branch_back(input_pair[stream_id], front_pair[stream_id]['normed'], front_pair[stream_id]['spread'], mod_pair[stream_id][:, 1], mlp_norm[stream_id][2]) for stream_id in range(2)]
            grads = [attn_norm[stream_id][2] for stream_id in range(2)]
            mod_rows = [jnp.stack([attn_norm[stream_id][0], attn_norm[stream_id][1], attn_parts[stream_id][0], mlp_norm[stream_id][0], mlp_norm[stream_id][1], mlp_parts[stream_id][0]], axis=1) for stream_id in range(2)]
            mod_list[layer_id] = jnp.stack([mod_rows[0][0], mod_rows[1][0]])
            qkv_acc = qkv_acc.at[layer_id].add(jnp.stack([product('btd,btkc->dkc', front_pair[stream_id]['hidden'], head_parts[stream_id][1]) for stream_id in range(2)]))
            out_acc = out_acc.at[layer_id].add(jnp.stack([attn_parts[stream_id][2] for stream_id in range(2)]))
            up_acc = up_acc.at[layer_id].add(jnp.stack([mlp_parts[stream_id][2] for stream_id in range(2)]))
            down_acc = down_acc.at[layer_id].add(jnp.stack([mlp_parts[stream_id][1] for stream_id in range(2)]))
            gain_acc = gain_acc.at[layer_id].add(jnp.stack([head_parts[stream_id][0] for stream_id in range(2)]))
        results = (streams[0][0].astype(jnp.bfloat16), streams[1][0].astype(jnp.bfloat16), grads[0][0].astype(jnp.bfloat16), grads[1][0].astype(jnp.bfloat16), jnp.stack(mod_list))
        return ((qkv_acc, out_acc, up_acc, down_acc, gain_acc), results)
    start = (jnp.zeros(qkv_weight.shape, jnp.float32), jnp.zeros(out_weight.shape, jnp.float32), jnp.zeros(up_weight.shape, jnp.float32), jnp.zeros(down_weight.shape, jnp.float32), jnp.zeros(norm_gain.shape, jnp.float32))
    totals, per_seq = lax.scan(one_sequence, start, (img_in, txt_in, cot_img, cot_txt, seq_mod))
    qkv_grad, out_grad, up_grad, down_grad, gain_grad = totals
    img_out, txt_out, img_grad, txt_grad, mod_rows_all = per_seq
    mod_grad = jnp.einsum('sm,sltkc->ltmkc', cond_act.astype(jnp.float32), mod_rows_all, precision=lax.Precision.HIGHEST)
    mod_next, mod_moment_next, mod_second_next = adam_step(mod_weight, mod_moment, mod_second, mod_grad)
    qkv_next, qkv_moment_next, qkv_second_next = adam_step(qkv_weight, qkv_moment, qkv_second, qkv_grad)
    out_next, out_moment_next, out_second_next = adam_step(out_weight, out_moment, out_second, out_grad)
    up_next, up_moment_next, up_second_next = adam_step(up_weight, up_moment, up_second, up_grad)
    down_next, down_moment_next, down_second_next = adam_step(down_weight, down_moment, down_second, down_grad)
    gain_next, gain_moment_next, gain_second_next = adam_step(norm_gain, gain_moment, gain_second, gain_grad)
    return (img_out, txt_out, img_grad, txt_grad, mod_grad, mod_next, mod_moment_next, mod_second_next, qkv_grad, qkv_next, qkv_moment_next, qkv_second_next, out_grad, out_next, out_moment_next, out_second_next, up_grad, up_next, up_moment_next, up_second_next, down_grad, down_next, down_moment_next, down_second_next, gain_grad, gain_next, gain_moment_next, gain_second_next)
```

```python
import functools
from types import SimpleNamespace as NS

import jax
import jax.numpy as jnp
from jax import lax
from jax.experimental import pallas as pl
from jax.experimental.pallas import tpu as pltpu
from jax.sharding import PartitionSpec as P

DP, CTX, TP = "dp", "ctx", "tp"
ROWS = (DP, CTX)
ALL = (DP, CTX, TP)

norm_eps = 1e-06
learn_rate = 0.004
beta_one = 0.9
beta_two = 0.999
adam_eps = 1e-08
decay_rate = 0.1
corr_one = 1.0 - beta_one**3
corr_two = 1.0 - beta_two**3

BF = jnp.bfloat16
F32 = jnp.float32


def product(pattern, former, latter):
    return jnp.einsum(pattern, former, latter, preferred_element_type=jnp.float32)


def layer_norm(values):
    center = values - jnp.mean(values, axis=-1, keepdims=True)
    spread = lax.rsqrt(jnp.mean(center * center, axis=-1, keepdims=True) + norm_eps)
    return (center * spread, spread)


def norm_back(incoming, normed, spread):
    return spread * (
        incoming
        - jnp.mean(incoming, axis=-1, keepdims=True)
        - normed * jnp.mean(incoming * normed, axis=-1, keepdims=True)
    )


def rms_norm(raw_rows):
    factor = lax.rsqrt(jnp.mean(raw_rows * raw_rows, axis=-1, keepdims=True) + norm_eps)
    return (raw_rows * factor, factor)


def rms_back(incoming, normed, factor):
    return factor * (incoming - normed * jnp.mean(incoming * normed, axis=-1, keepdims=True))


def gelu_tanh(values):
    return jax.nn.gelu(values, approximate=True)


def adam_step(weight, moment, second, gradient):
    new_moment = beta_one * moment + (1.0 - beta_one) * gradient
    new_second = beta_two * second + (1.0 - beta_two) * gradient * gradient
    update = (
        new_moment / corr_one / (jnp.sqrt(new_second / corr_two) + adam_eps) + decay_rate * weight
    )
    return (weight - learn_rate * update, new_moment, new_second)


def modulate(normed, shift_vec, scale_vec):
    return (normed * (1.0 + scale_vec[:, None, :]) + shift_vec[:, None, :]).astype(jnp.bfloat16)


def stream_front(inputs, modulation, qkv_part, gain_pair):
    values = inputs.astype(jnp.float32)
    normed, spread = layer_norm(values)
    hidden = modulate(normed, modulation[:, 0], modulation[:, 1])
    packed = product("btd,dkc->btkc", hidden, qkv_part)
    packed = packed.reshape(packed.shape[0], packed.shape[1], 3, -1, gain_pair.shape[-1])
    q_hat, q_factor = rms_norm(packed[:, :, 0])
    k_hat, k_factor = rms_norm(packed[:, :, 1])
    return NS(        values=values,
        normed=normed,
        spread=spread,
        hidden=hidden,
        q_hat=q_hat,
        q_factor=q_factor,
        k_hat=k_hat,
        k_factor=k_factor,
        queries=(q_hat * gain_pair[0]).astype(jnp.bfloat16),
        key_rows=(k_hat * gain_pair[1]).astype(jnp.bfloat16),
        value_rows=packed[:, :, 2].astype(jnp.bfloat16),)


def mlp_front(resid, modulation, up_part):
    normed, spread = layer_norm(resid)
    hidden = modulate(normed, modulation[:, 3], modulation[:, 4])
    pre_act = product("btd,df->btf", hidden, up_part)
    activated = gelu_tanh(pre_act).astype(jnp.bfloat16)
    return NS(        normed=normed,
        spread=spread,
        hidden=hidden,
        pre_act=pre_act,
        activated=activated,)


def attend(query_all, key_all, value_all, scale_factor):
    scores = product("bqhd,bkhd->bhqk", query_all, key_all) * scale_factor
    row_peak = jnp.max(scores, axis=-1, keepdims=True)
    log_total = row_peak + jnp.log(jnp.sum(jnp.exp(scores - row_peak), axis=-1, keepdims=True))
    attn_probs = jnp.exp(scores - log_total).astype(jnp.bfloat16)
    attended = product("bhqk,bkhd->bqhd", attn_probs, value_all)
    return (attended, log_total)


def attend_back(
    grad_att, query_all, key_all, value_all, attended, log_total, scale_factor, split_at
):
    row_delta = jnp.sum(grad_att.astype(jnp.float32) * attended, axis=-1)
    scores = product("bqhd,bkhd->bhqk", query_all, key_all) * scale_factor
    attn_probs = jnp.exp(scores - log_total)
    prob_grad = product("bqhd,bkhd->bhqk", grad_att, value_all)
    score_grad = (
        attn_probs * (prob_grad - jnp.transpose(row_delta, (0, 2, 1))[..., None]) * scale_factor
    ).astype(jnp.bfloat16)
    probs_low = attn_probs.astype(jnp.bfloat16)
    query_grad = product("bhqk,bkhd->bqhd", score_grad, key_all)
    key_first = product("bhqk,bqhd->bkhd", score_grad[:, :, :split_at], query_all[:, :split_at])
    key_second = product("bhqk,bqhd->bkhd", score_grad[:, :, split_at:], query_all[:, split_at:])
    value_first = product("bhqk,bqhd->bkhd", probs_low[:, :, :split_at], grad_att[:, :split_at])
    value_second = product("bhqk,bqhd->bkhd", probs_low[:, :, split_at:], grad_att[:, split_at:])
    return (query_grad, key_first, key_second, value_first, value_second)


def mlp_back(grad_out, modulation, mlp_parts, down_out, up_part, down_part):
    gate_two = jnp.sum(grad_out * down_out, axis=1)
    branch = (grad_out * modulation[:, 5][:, None, :]).astype(jnp.bfloat16)
    act_grad = product("btd,fd->btf", branch, down_part)
    down_term = product("btf,btd->fd", mlp_parts.activated, branch)
    pre_grad = jax.vjp(gelu_tanh, mlp_parts.pre_act)[1](act_grad)[0].astype(jnp.bfloat16)
    up_term = product("btd,btf->df", mlp_parts.hidden, pre_grad)
    hidden_part = product("btf,df->btd", pre_grad, up_part)
    return (gate_two, down_term, up_term, hidden_part)


def norm_branch_back(hidden_grad, normed, spread, scale_vec, residual_grad):
    shift_grad = jnp.sum(hidden_grad, axis=1)
    scale_grad = jnp.sum(hidden_grad * normed, axis=1)
    total = residual_grad + norm_back(hidden_grad * (1.0 + scale_vec[:, None, :]), normed, spread)
    return (shift_grad, scale_grad, total)


def attention_branch_back(resid_grad, modulation, proj, flat_rows, out_part):
    gate_one = jnp.sum(resid_grad * proj, axis=1)
    branch = (resid_grad * modulation[:, 2][:, None, :]).astype(jnp.bfloat16)
    att_grad = product("btd,cd->btc", branch, out_part)
    out_term = product("btc,btd->cd", flat_rows, branch)
    return (gate_one, att_grad, out_term)


def head_back(query_grad, key_grad, value_grad, front, gain_pair):
    gain_term = jnp.stack(
        [
            jnp.sum(query_grad * front.q_hat, axis=(0, 1, 2)),
            jnp.sum(key_grad * front.k_hat, axis=(0, 1, 2)),
        ]
    )
    q_raw = rms_back(query_grad * gain_pair[0], front.q_hat, front.q_factor)
    k_raw = rms_back(key_grad * gain_pair[1], front.k_hat, front.k_factor)
    packed = jnp.stack([q_raw, k_raw, value_grad], axis=2)
    packed = packed.reshape(packed.shape[0], packed.shape[1], 3, -1).astype(jnp.bfloat16)
    return (gain_term, packed)


def gathered_body(
    img_in,
    txt_in,
    cond,
    mod_weight,
    qkv_weight,
    out_weight,
    up_weight,
    down_weight,
    norm_gain,
    cot_img,
    cot_txt,
    mod_moment,
    qkv_moment,
    out_moment,
    up_moment,
    down_moment,
    gain_moment,
    mod_second,
    qkv_second,
    out_second,
    up_second,
    down_second,
    gain_second,
):
    ctx_count = lax.axis_size(CTX)
    tp_count = lax.axis_size(TP)
    seq_dev = img_in.shape[0]
    img_dev = img_in.shape[1]
    txt_rows = txt_in.shape[1]
    img_total = img_dev * ctx_count
    layer_count = qkv_weight.shape[0]
    head_dim = norm_gain.shape[-1]
    scale_factor = head_dim ** (-0.5)
    seq_start = lax.axis_index(DP) * seq_dev
    ctx_start = lax.axis_index(CTX) * img_dev
    cond_act = jax.nn.silu(cond.astype(jnp.float32)).astype(jnp.bfloat16)
    mod_part = product("sm,ltmkc->ltskc", cond_act, mod_weight.astype(jnp.bfloat16))
    all_mod = lax.psum(mod_part, ALL)
    own_mod = lax.dynamic_slice_in_dim(all_mod, seq_start, seq_dev, 2)

    def gather_weights(layer_id):
        return (
            lax.all_gather(
                qkv_weight[layer_id].astype(jnp.bfloat16), ROWS, axis=1, tiled=True
            ),
            lax.all_gather(
                out_weight[layer_id].astype(jnp.bfloat16), ROWS, axis=2, tiled=True
            ),
            lax.all_gather(
                up_weight[layer_id].astype(jnp.bfloat16), ROWS, axis=1, tiled=True
            ),
            lax.all_gather(
                down_weight[layer_id].astype(jnp.bfloat16), ROWS, axis=2, tiled=True
            ),
        )

    def joined_keys(front_pair):
        remote_keys, remote_values = (
            lax.all_gather(front_pair[0].key_rows, CTX, axis=1, tiled=True),
            lax.all_gather(front_pair[0].value_rows, CTX, axis=1, tiled=True),
        )
        key_all = jnp.concatenate([remote_keys, front_pair[1].key_rows], axis=1)
        value_all = jnp.concatenate([remote_values, front_pair[1].value_rows], axis=1)
        return (key_all, value_all)

    streams = [img_in, txt_in]
    layer_id = 0
    full_qkv, full_out, full_up, full_down = gather_weights(layer_id)
    mod_pair = [own_mod[layer_id, 0], own_mod[layer_id, 1]]
    front_pair = [
        stream_front(
            streams[stream_id],
            mod_pair[stream_id],
            full_qkv[stream_id],
            norm_gain[layer_id, stream_id],
        )
        for stream_id in range(2)
    ]
    key_all, value_all = joined_keys(front_pair)
    query_all = jnp.concatenate([front_pair[0].queries, front_pair[1].queries], axis=1)
    attended, log_total = attend(query_all, key_all, value_all, scale_factor)
    attended_low = attended.astype(jnp.bfloat16)
    flat_pair = [
        attended_low[:, :img_dev].reshape(seq_dev, img_dev, -1),
        attended_low[:, img_dev:].reshape(seq_dev, txt_rows, -1),
    ]
    proj_img = lax.psum(
        product("btc,cd->btd", flat_pair[0], full_out[0]).astype(jnp.bfloat16), TP
    ).astype(jnp.float32)
    proj_txt = lax.psum(
        product("btc,cd->btd", flat_pair[1], full_out[1]).astype(jnp.bfloat16), TP
    ).astype(jnp.float32)
    proj_pair = [proj_img, proj_txt]
    resid_pair = [
        front_pair[stream_id].values
        + mod_pair[stream_id][:, 2][:, None, :] * proj_pair[stream_id]
        for stream_id in range(2)
    ]
    mlp_pair = [
        mlp_front(resid_pair[stream_id], mod_pair[stream_id], full_up[stream_id])
        for stream_id in range(2)
    ]
    down_img = lax.psum(
        product("btf,fd->btd", mlp_pair[0].activated, full_down[0]).astype(jnp.bfloat16), TP
    ).astype(jnp.float32)
    down_txt = lax.psum(
        product("btf,fd->btd", mlp_pair[1].activated, full_down[1]).astype(jnp.bfloat16), TP
    ).astype(jnp.float32)
    down_pair = [down_img, down_txt]
    streams = [
        resid_pair[stream_id] + mod_pair[stream_id][:, 5][:, None, :] * down_pair[stream_id]
        for stream_id in range(2)
    ]
    stored = [
        NS(            weights=(full_qkv, full_out, full_up, full_down),
            front=front_pair,
            key_all=key_all,
            value_all=value_all,
            query_all=query_all,
            attended=attended,
            log_total=log_total,
            flat=flat_pair,
            proj=proj_pair,
            mlp=mlp_pair,
            down=down_pair,)
    ]
    grads = [cot_img.astype(jnp.float32), cot_txt.astype(jnp.float32)]
    mod_terms = [None] * layer_count
    gain_terms = [None] * layer_count
    owned_grads = [None] * layer_count
    for layer_id in reversed(range(layer_count)):
        saved = stored[layer_id]
        mod_pair = [own_mod[layer_id, 0], own_mod[layer_id, 1]]
        front_pair = saved.front
        full_qkv, full_out, full_up, full_down = gather_weights(layer_id)
        key_all, value_all = joined_keys(front_pair)
        mlp_parts = [
            mlp_back(
                grads[stream_id],
                mod_pair[stream_id],
                saved.mlp[stream_id],
                saved.down[stream_id],
                full_up[stream_id],
                full_down[stream_id],
            )
            for stream_id in range(2)
        ]
        hidden_img, hidden_txt = (
            lax.psum(mlp_parts[0][3].astype(jnp.bfloat16), TP).astype(jnp.float32),
            lax.psum(mlp_parts[1][3].astype(jnp.bfloat16), TP).astype(jnp.float32),
        )
        hidden_pair = [hidden_img, hidden_txt]
        mlp_norm = [
            norm_branch_back(
                hidden_pair[stream_id],
                saved.mlp[stream_id].normed,
                saved.mlp[stream_id].spread,
                mod_pair[stream_id][:, 4],
                grads[stream_id],
            )
            for stream_id in range(2)
        ]
        attn_parts = [
            attention_branch_back(
                mlp_norm[stream_id][2],
                mod_pair[stream_id],
                saved.proj[stream_id],
                saved.flat[stream_id],
                full_out[stream_id],
            )
            for stream_id in range(2)
        ]
        grad_att = jnp.concatenate(
            [
                attn_parts[0][1].reshape(seq_dev, img_dev, -1, head_dim),
                attn_parts[1][1].reshape(seq_dev, txt_rows, -1, head_dim),
            ],
            axis=1,
        ).astype(jnp.bfloat16)
        query_grad, key_first, key_second, value_first, value_second = attend_back(
            grad_att,
            saved.query_all,
            key_all,
            value_all,
            saved.attended,
            saved.log_total,
            scale_factor,
            img_dev,
        )
        key_img_sum, value_img_sum = (
            lax.psum_scatter(
                key_first[:, :img_total].astype(jnp.bfloat16),
                CTX,
                scatter_dimension=1,
                tiled=True,
            ).astype(jnp.float32),
            lax.psum_scatter(
                value_first[:, :img_total].astype(jnp.bfloat16),
                CTX,
                scatter_dimension=1,
                tiled=True,
            ).astype(jnp.float32),
        )
        key_txt_sum, value_txt_sum = (
            lax.psum(key_first[:, img_total:].astype(jnp.bfloat16), CTX).astype(jnp.float32),
            lax.psum(value_first[:, img_total:].astype(jnp.bfloat16), CTX).astype(jnp.float32),
        )
        key_pair = [
            key_img_sum
            + lax.dynamic_slice_in_dim(key_second[:, :img_total], ctx_start, img_dev, 1),
            key_txt_sum + key_second[:, img_total:],
        ]
        value_pair = [
            value_img_sum
            + lax.dynamic_slice_in_dim(value_second[:, :img_total], ctx_start, img_dev, 1),
            value_txt_sum + value_second[:, img_total:],
        ]
        query_pair = [query_grad[:, :img_dev], query_grad[:, img_dev:]]
        head_parts = [
            head_back(
                query_pair[stream_id],
                key_pair[stream_id],
                value_pair[stream_id],
                front_pair[stream_id],
                norm_gain[layer_id, stream_id],
            )
            for stream_id in range(2)
        ]
        input_img, input_txt = (
            lax.psum(
                product("btkc,dkc->btd", head_parts[0][1], full_qkv[0]).astype(jnp.bfloat16), TP
            ).astype(jnp.float32),
            lax.psum(
                product("btkc,dkc->btd", head_parts[1][1], full_qkv[1]).astype(jnp.bfloat16), TP
            ).astype(jnp.float32),
        )
        input_pair = [input_img, input_txt]
        attn_norm = [
            norm_branch_back(
                input_pair[stream_id],
                front_pair[stream_id].normed,
                front_pair[stream_id].spread,
                mod_pair[stream_id][:, 1],
                mlp_norm[stream_id][2],
            )
            for stream_id in range(2)
        ]
        grads = [attn_norm[stream_id][2] for stream_id in range(2)]
        mod_rows = [
            jnp.stack(
                [
                    attn_norm[stream_id][0],
                    attn_norm[stream_id][1],
                    attn_parts[stream_id][0],
                    mlp_norm[stream_id][0],
                    mlp_norm[stream_id][1],
                    mlp_parts[stream_id][0],
                ],
                axis=1,
            )
            for stream_id in range(2)
        ]
        mod_terms[layer_id] = jnp.stack([mod_rows[0], mod_rows[1] / ctx_count]) / tp_count
        gain_terms[layer_id] = jnp.stack([head_parts[0][0], head_parts[1][0] / ctx_count])
        qkv_stack = jnp.stack(
            [
                product("btd,btkc->dkc", front_pair[stream_id].hidden, head_parts[stream_id][1])
                for stream_id in range(2)
            ]
        )
        out_stack = jnp.stack([attn_parts[stream_id][2] for stream_id in range(2)])
        up_stack = jnp.stack([mlp_parts[stream_id][2] for stream_id in range(2)])
        down_stack = jnp.stack([mlp_parts[stream_id][1] for stream_id in range(2)])
        qkv_term = jnp.concatenate([qkv_stack[0:1], qkv_stack[1:2] / ctx_count])
        out_term = jnp.concatenate([out_stack[0:1], out_stack[1:2] / ctx_count])
        up_term = jnp.concatenate([up_stack[0:1], up_stack[1:2] / ctx_count])
        down_term = jnp.concatenate([down_stack[0:1], down_stack[1:2] / ctx_count])
        owned = (
            lax.psum_scatter(
                qkv_term.astype(jnp.bfloat16), ROWS, scatter_dimension=1, tiled=True
            ).astype(jnp.float32),
            lax.psum_scatter(
                out_term.astype(jnp.bfloat16), ROWS, scatter_dimension=2, tiled=True
            ).astype(jnp.float32),
            lax.psum_scatter(
                up_term.astype(jnp.bfloat16), ROWS, scatter_dimension=1, tiled=True
            ).astype(jnp.float32),
            lax.psum_scatter(
                down_term.astype(jnp.bfloat16), ROWS, scatter_dimension=2, tiled=True
            ).astype(jnp.float32),
        )
        owned_grads[layer_id] = owned
    mod_local = jnp.stack(mod_terms)
    mod_zero = jnp.zeros(
        (layer_count, 2, seq_dev * lax.axis_size(DP)) + mod_local.shape[3:], jnp.float32
    )
    mod_term = lax.dynamic_update_slice_in_dim(mod_zero, mod_local, seq_start, 2)
    mod_full, gain_grad = lax.psum((mod_term, jnp.stack(gain_terms)), ALL)
    mod_grad = jnp.einsum(
        "sm,ltskc->ltmkc", cond_act.astype(jnp.float32), mod_full, precision=lax.Precision.HIGHEST
    )
    qkv_grad = jnp.stack([owned_grads[0][0]])
    out_grad = jnp.stack([owned_grads[0][1]])
    up_grad = jnp.stack([owned_grads[0][2]])
    down_grad = jnp.stack([owned_grads[0][3]])
    mod_next, mod_moment_next, mod_second_next = adam_step(
        mod_weight, mod_moment, mod_second, mod_grad
    )
    qkv_next, qkv_moment_next, qkv_second_next = adam_step(
        qkv_weight, qkv_moment, qkv_second, qkv_grad
    )
    out_next, out_moment_next, out_second_next = adam_step(
        out_weight, out_moment, out_second, out_grad
    )
    up_next, up_moment_next, up_second_next = adam_step(up_weight, up_moment, up_second, up_grad)
    down_next, down_moment_next, down_second_next = adam_step(
        down_weight, down_moment, down_second, down_grad
    )
    gain_next, gain_moment_next, gain_second_next = adam_step(
        norm_gain, gain_moment, gain_second, gain_grad
    )
    return (
        streams[0].astype(jnp.bfloat16),
        streams[1].astype(jnp.bfloat16),
        grads[0].astype(jnp.bfloat16),
        grads[1].astype(jnp.bfloat16),
        mod_grad,
        mod_next,
        mod_moment_next,
        mod_second_next,
        qkv_grad,
        qkv_next,
        qkv_moment_next,
        qkv_second_next,
        out_grad,
        out_next,
        out_moment_next,
        out_second_next,
        up_grad,
        up_next,
        up_moment_next,
        up_second_next,
        down_grad,
        down_next,
        down_moment_next,
        down_second_next,
        gain_grad,
        gain_next,
        gain_moment_next,
        gain_second_next,
    )


class Place:
    def __init__(self, zn):
        self.zn = zn
        self.d, self.c, self.t = lax.axis_index(DP), lax.axis_index(CTX), lax.axis_index(TP)
        self.y, self.k = self.d // 2, self.d % 2
        self.d_core = self.y * 2 + (1 - self.k)
        self.d_y = (1 - self.y) * 2 + self.k
        self.t_x = 1 - self.t

    def ahead(self, step):
        return (self.c + step) % self.zn

    def behind(self, step):
        return (self.c + self.zn - step) % self.zn

    def greet(self, core=True, y=True, x=True, z=True):
        sem = pltpu.get_barrier_semaphore()
        count = 0
        for wanted, where in ((x, {TP: self.t_x}), (core, {DP: self.d_core}), (y, {DP: self.d_y})):
            if wanted:
                pl.semaphore_signal(sem, inc=1, device_id=where, device_id_type=pl.DeviceIdType.MESH)
                count += 1
        if z:
            for step in range(1, self.zn):
                pl.semaphore_signal(
                    sem, inc=1, device_id={CTX: self.ahead(step)}, device_id_type=pl.DeviceIdType.MESH
                )
                count += 1
        pl.semaphore_wait(sem, count)


def remote(src, dst, send, recv, where):
    copy = pltpu.make_async_remote_copy(
        src_ref=src,
        dst_ref=dst,
        send_sem=send,
        recv_sem=recv,
        device_id=where,
        device_id_type=pl.DeviceIdType.MESH,
    )
    copy.start()
    return copy


def local(src, dst, sem):
    copy = pltpu.make_async_copy(src, dst, sem)
    copy.start()
    return copy


HBM = pl.BlockSpec(memory_space=pl.ANY)
VMEM = pl.BlockSpec(memory_space=pltpu.VMEM)
DMA = pltpu.SemaphoreType.DMA


def call(kernel, ident, ins, outs, scratch, args, flops=0):
    return pl.pallas_call(
        kernel,
        out_shape=[shape for shape, _ in outs],
        in_specs=ins,
        out_specs=[spec for _, spec in outs],
        scratch_shapes=scratch,
        compiler_params=pltpu.CompilerParams(
            collective_id=ident, has_side_effects=True, vmem_limit_bytes=60 * 1024 * 1024
        ),
    )(*args)


def shaped(shape, dtype):
    return jax.ShapeDtypeStruct(shape, dtype)


def spread_kernel(
    zn, wa, wu, wd, xi, ci, mp, ga, gu, gd, xo, co, mod,
    bw, bx, my, m2, mc, m1, mx, slots,
    zs, zr, ys, yr, cs, cr, xs, xr, ms, mr, loc,
):
    me = Place(zn)
    me.greet()
    d, c, t, y, k = me.d, me.c, me.t, me.y, me.k
    outs = (ga, gu, gd)
    own = []
    bounce = []
    for kind, w in enumerate((wa, wu, wd)):
        bounce.append(local(w.at[c], bw.at[kind], loc.at[kind]))
    for act, a in enumerate((xi, ci)):
        bounce.append(local(a, bx.at[act], loc.at[3 + act]))
    pending = []
    m_y = remote(mp.at[pl.ds((1 - y) * 2, 2)], my, ms.at[0], mr.at[0], {DP: me.d_y})
    zcopies = {}

    def send_tokens(act, a, o):
        zcopies[6 + act] = [
            remote(a.at[t], o.at[c, t], zs.at[6 + act, s - 1], zr.at[6 + act, s - 1], {CTX: me.ahead(s)})
            for s in range(1, zn)
        ]

    def send_weights(kind, w):
        for st in range(2):
            zcopies[kind * 2 + st] = [
                remote(
                    w.at[me.ahead(s), st],
                    outs[kind].at[st, d * zn + c],
                    zs.at[kind * 2 + st, s - 1],
                    zr.at[kind * 2 + st, s - 1],
                    {CTX: me.ahead(s)},
                )
                for s in range(1, zn)
            ]

    send_tokens(0, xi, xo)
    send_weights(0, wa)
    send_weights(1, wu)
    send_weights(2, wd)
    send_tokens(1, ci, co)

    for kind in range(3):
        bounce[kind].wait()
        for st in range(2):
            own.append(local(bw.at[kind, st], outs[kind].at[st, d * zn + c], loc.at[5 + kind * 2 + st]))
    for act, o in enumerate((xo, co)):
        bounce[3 + act].wait()
        own.append(local(bx.at[act], o.at[c], loc.at[11 + act]))

    m_y.wait()
    m2[...] = mp[pl.ds(y * 2, 2)] + my[...]
    m_c = remote(m2.at[1 - k], mc, ms.at[1], mr.at[1], {DP: me.d_core})
    m_c.wait()
    m1[...] = m2[k] + mc[...]
    m_x = remote(m1, mx, ms.at[2], mr.at[2], {TP: me.t_x})
    m_x.wait()
    slots[c] = m1[...] + mx[...]
    m_z = [
        remote(slots.at[c], slots.at[c], ms.at[2 + s], mr.at[2 + s], {CTX: me.ahead(s)})
        for s in range(1, zn)
    ]

    def forward_tokens(act, o):
        for s in range(1, zn):
            zcopies[6 + act][s - 1].wait()
            src = me.behind(s)
            pending.append(
                remote(o.at[src, t], o.at[src, t], xs.at[act, s - 1], xr.at[act, s - 1], {TP: me.t_x})
            )

    forward_tokens(0, xo)
    ycopies = []
    for chunk in range(6):
        kind, st = divmod(chunk, 2)
        g = outs[kind]
        for copy in zcopies[chunk]:
            copy.wait()
        own[chunk].wait()
        mine = g.at[st, pl.ds(d * zn, zn)]
        ycopies.append(remote(mine, mine, ys.at[chunk], yr.at[chunk], {DP: me.d_y}))
        pending.append(remote(mine, mine, cs.at[chunk, 0], cr.at[chunk, 0], {DP: me.d_core}))
        if chunk:
            pass_on(me, outs, chunk - 1, ycopies, pending, cs, cr)
        if chunk == 1:
            for copy in m_z:
                copy.wait()
            total = slots[0]
            for z in range(1, zn):
                total = total + slots[z]
            mod[...] = total
    forward_tokens(1, co)
    pass_on(me, outs, 5, ycopies, pending, cs, cr)
    for copy in pending:
        copy.wait()
    for copy in own[6:]:
        copy.wait()


def pass_on(me, outs, chunk, ycopies, pending, cs, cr):
    kind, st = divmod(chunk, 2)
    ycopies[chunk].wait()
    there = outs[kind].at[st, pl.ds(me.d_y * me.zn, me.zn)]
    pending.append(remote(there, there, cs.at[chunk, 1], cr.at[chunk, 1], {DP: me.d_core}))


def spread(zn, wa, wu, wd, xi, ci, mp):
    rows, width = wa.shape[2:]
    half, dim = xi.shape[1:]
    lines = mp.shape[1]
    weight = shaped((2, 4 * zn, rows, width), BF)
    token = shaped((zn, 2, half, dim), BF)
    return call(
        functools.partial(spread_kernel, zn),
        0,
        [HBM] * 5 + [VMEM],
        [(weight, HBM)] * 3 + [(token, HBM)] * 2 + [(shaped((lines, 128), F32), VMEM)],
        [
            pltpu.VMEM((3, 2, rows, width), BF),
            pltpu.VMEM((2, 2, half, dim), BF),
            pltpu.VMEM((2, lines, 128), F32),
            pltpu.VMEM((2, lines, 128), F32),
            pltpu.VMEM((lines, 128), F32),
            pltpu.VMEM((lines, 128), F32),
            pltpu.VMEM((lines, 128), F32),
            pltpu.VMEM((zn, lines, 128), F32),
            DMA((8, zn)), DMA((8, zn)), DMA((6,)), DMA((6,)), DMA((6, 2)), DMA((6, 2)),
            DMA((2, zn)), DMA((2, zn)), DMA((2 + zn,)), DMA((2 + zn,)), DMA((13,)),
        ],
        (wa, wu, wd, xi, ci, mp),
    )


CHUNK = 16


def sum_start(me, arrays, own, recvx, xs, xr, loc):
    order = list(range(1, me.zn)) + [0]
    copies = {}
    for a, parts in enumerate(arrays):
        for s in order:
            zb = me.ahead(s)
            at = 0
            group = []
            for p, part in enumerate(parts):
                n = part.shape[2]
                group.append(
                    remote(
                        part.at[zb, me.t_x],
                        recvx.at[a, s, pl.ds(at, n)],
                        xs.at[a, s, p],
                        xr.at[a, s, p],
                        {TP: me.t_x},
                    )
                )
                group.append(local(part.at[zb, me.t], own.at[a, s, pl.ds(at, n)], loc.at[a, s, p]))
                at += n
            copies[a, s] = group
    return copies


def sum_x(me, a, copies, own, recvx, sumb, recvz, total, zs, zr):
    rows = own.shape[2]
    out = []
    for s in list(range(1, me.zn)) + [0]:
        for copy in copies[a, s]:
            copy.wait()
        if s:

            @pl.loop(0, rows // CHUNK)
            def _(i):
                at = pl.ds(pl.multiple_of(i * CHUNK, CHUNK), CHUNK)
                sumb[a, s, at] = (own[a, s, at].astype(F32) + recvx[a, s, at].astype(F32)).astype(BF)

            out.append(
                remote(sumb.at[a, s], recvz.at[a, s], zs.at[a, s], zr.at[a, s], {CTX: me.ahead(s)})
            )
        else:

            @pl.loop(0, rows // CHUNK)
            def _(i):
                at = pl.ds(pl.multiple_of(i * CHUNK, CHUNK), CHUNK)
                total[a, at] = own[a, s, at].astype(F32) + recvx[a, s, at].astype(F32)

    return out


def sum_z(me, a, copies, recvz, total):
    for copy in copies:
        copy.wait()
    rows = total.shape[1]

    @pl.loop(0, rows // CHUNK)
    def _(i):
        at = pl.ds(pl.multiple_of(i * CHUNK, CHUNK), CHUNK)
        value = total[a, at]
        for s in range(1, me.zn):
            value = value + recvz[a, s, at].astype(F32)
        total[a, at] = value


def share_start(me, block, outs, sizes, zs, zr, xs, xr, loc):
    copies = []
    at = 0
    for p, (o, n) in enumerate(zip(outs, sizes)):
        src = block.at[pl.ds(at, n)]
        at += n
        dst = o.at[me.c, me.t]
        group = [
            remote(src, dst, zs.at[p, s], zr.at[p, s], {CTX: me.ahead(s)}) for s in range(1, me.zn)
        ]
        group.append(remote(src, dst, xs.at[p, 0], xr.at[p, 0], {TP: me.t_x}))
        group.append(local(src, dst, loc.at[p]))
        copies.append(group)
    return copies


def share_end(me, copies, outs, xs, xr):
    passed = []
    for s in range(1, me.zn):
        src = me.behind(s)
        for p, o in enumerate(outs):
            copies[p][s - 1].wait()
            passed.append(
                remote(o.at[src, me.t], o.at[src, me.t], xs.at[p, s], xr.at[p, s], {TP: me.t_x})
            )
    for group in copies:
        for copy in group[me.zn - 1 :]:
            copy.wait()
    for copy in passed:
        copy.wait()


def row_loops(sizes, fn):
    at = 0
    for stream, n in enumerate(sizes):

        @pl.loop(0, n // CHUNK)
        def _(i, at=at, stream=stream):
            fn(stream, pl.ds(pl.multiple_of(at + i * CHUNK, CHUNK), CHUNK))

        at += n


def line(mod, stream, which):
    return mod[stream * 6 + which][None, :]


def sum_scratch(count, zn, rows, dim):
    return [
        pltpu.VMEM((count, zn, rows, dim), BF),
        pltpu.VMEM((count, zn, rows, dim), BF),
        pltpu.VMEM((count, zn, rows, dim), BF),
        pltpu.VMEM((count, zn, rows, dim), BF),
        pltpu.VMEM((count, rows, dim), F32),
        DMA((count, zn, 2)), DMA((count, zn, 2)), DMA((count, zn, 2)),
        DMA((count, zn)), DMA((count, zn)),
    ]


def share_scratch(zn, rows, dim):
    return [
        pltpu.VMEM((rows, dim), BF),
        DMA((2, zn)), DMA((2, zn)), DMA((2, zn)), DMA((2, zn)), DMA((2,)),
    ]


def middle_kernel(
    zn, sizes, pi, pt, xr_rows, mod, hi, ht, resid, proj,
    own, recvx, sumb, recvz, total, sxs, sxr, sloc, szs, szr,
    hb, gzs, gzr, gxs, gxr, gloc,
):
    me = Place(zn)
    me.greet(core=False, y=False)
    copies = sum_start(me, [(pi, pt)], own, recvx, sxs, sxr, sloc)
    zc = sum_x(me, 0, copies, own, recvx, sumb, recvz, total, szs, szr)
    sum_z(me, 0, zc, recvz, total)

    def rows(stream, at):
        p = total[0, at]
        proj[at] = p
        value = xr_rows[at].astype(F32) + line(mod, stream, 2) * p
        resid[at] = value
        normed, _ = layer_norm(value)
        hb[at] = (normed * (1.0 + line(mod, stream, 4)) + line(mod, stream, 3)).astype(BF)

    row_loops(sizes, rows)
    copies = share_start(me, hb, (hi, ht), sizes, gzs, gzr, gxs, gxr, gloc)
    share_end(me, copies, (hi, ht), gxs, gxr)


def middle(zn, sizes, pi, pt, rows, mod):
    dim = rows.shape[1]
    total = sum(sizes)
    return call(
        functools.partial(middle_kernel, zn, sizes),
        1,
        [HBM, HBM, VMEM, VMEM],
        [
            (shaped(pi.shape, BF), HBM),
            (shaped(pt.shape, BF), HBM),
            (shaped((total, dim), F32), VMEM),
            (shaped((total, dim), F32), VMEM),
        ],
        sum_scratch(1, zn, total, dim) + share_scratch(zn, total, dim),
        (pi, pt, rows, mod),
    )


def turn_kernel(
    zn, sizes, hi, ht, mi, mt, resid, proj, cot, mod, bi, bt, out, rgrad, sums,
    own, recvx, sumb, recvz, total, sxs, sxr, sloc, szs, szr,
    bb, gzs, gzr, gxs, gxr, gloc,
):
    me = Place(zn)
    me.greet(core=False, y=False)
    copies = sum_start(me, [(hi, ht), (mi, mt)], own, recvx, sxs, sxr, sloc)
    zh = sum_x(me, 0, copies, own, recvx, sumb, recvz, total, szs, szr)
    sums[...] = jnp.zeros_like(sums)
    sum_z(me, 0, zh, recvz, total)

    def rows(stream, at):
        h = total[0, at]
        normed, spread_ = layer_norm(resid[at])
        g = cot[at].astype(F32)
        value = g + norm_back(h * (1.0 + line(mod, stream, 4)), normed, spread_)
        rgrad[at] = value
        bb[at] = (value * line(mod, stream, 2)).astype(BF)
        sums[stream, 0] += jnp.sum(value * proj[at], axis=0)
        sums[stream, 1] += jnp.sum(h, axis=0)
        sums[stream, 2] += jnp.sum(h * normed, axis=0)

    row_loops(sizes, rows)
    shared = share_start(me, bb, (bi, bt), sizes, gzs, gzr, gxs, gxr, gloc)
    zm = sum_x(me, 1, copies, own, recvx, sumb, recvz, total, szs, szr)
    share_end(me, shared, (bi, bt), gxs, gxr)
    sum_z(me, 1, zm, recvz, total)

    def tail(stream, at):
        m = total[1, at]
        out[at] = (resid[at] + line(mod, stream, 5) * m).astype(BF)
        sums[stream, 3] += jnp.sum(cot[at].astype(F32) * m, axis=0)

    row_loops(sizes, tail)


def turn(zn, sizes, hi, ht, mi, mt, resid, proj, cot, mod):
    total, dim = resid.shape
    return call(
        functools.partial(turn_kernel, zn, sizes),
        2,
        [HBM] * 4 + [VMEM] * 4,
        [
            (shaped(hi.shape, BF), HBM),
            (shaped(ht.shape, BF), HBM),
            (shaped((total, dim), BF), VMEM),
            (shaped((total, dim), F32), VMEM),
            (shaped((2, 4, dim), F32), VMEM),
        ],
        sum_scratch(2, zn, total, dim) + share_scratch(zn, total, dim),
        (hi, ht, mi, mt, resid, proj, cot, mod),
    )


def finish_kernel(
    zn, sizes, ai, at_, x_rows, rgrad, out, sums, gains, mod, oi, ot, gsum,
    own, recvx, sumb, recvz, total, sxs, sxr, sloc, szs, szr,
    ob, msum, mx, slots, xs, xr, zs, zr, fs, fr, loc, ms, mr,
):
    me = Place(zn)
    me.greet()
    c, t = me.c, me.t
    n_img, n_txt = sizes
    copies = sum_start(me, [(ai, at_)], own, recvx, sxs, sxr, sloc)

    def keep(stream, at):
        ob[0, at] = out[at]

    row_loops(sizes, keep)
    zc = sum_x(me, 0, copies, own, recvx, sumb, recvz, total, szs, szr)
    msum[...] = jnp.zeros_like(msum)
    sum_z(me, 0, zc, recvz, total)

    def rows(stream, at):
        h = total[0, at]
        normed, spread_ = layer_norm(x_rows[at].astype(F32))
        value = rgrad[at] + norm_back(h * (1.0 + line(mod, stream, 1)), normed, spread_)
        ob[1, at] = value.astype(BF)
        msum[stream * 6] += jnp.sum(h, axis=0)
        msum[stream * 6 + 1] += jnp.sum(h * normed, axis=0)

    row_loops(sizes, rows)
    for stream in range(2):
        for which in range(4):
            msum[stream * 6 + 2 + which] = sums[stream, which]
    msum[12] = gains[0]
    m_x = remote(msum, mx, ms.at[0], mr.at[0], {TP: me.t_x})
    img = ob.at[:, pl.ds(0, n_img)]
    txt = ob.at[:, pl.ds(n_img, n_txt)]
    done = [
        remote(img, oi.at[:, t], xs.at[0], xr.at[0], {TP: me.t_x}),
        remote(txt, ot.at[:, c, t], xs.at[1], xr.at[1], {TP: me.t_x}),
        local(img, oi.at[:, t], loc.at[0]),
        local(txt, ot.at[:, c, t], loc.at[1]),
    ]
    over_z = [
        remote(txt, ot.at[:, c, t], zs.at[s], zr.at[s], {CTX: me.ahead(s)}) for s in range(1, zn)
    ]
    m_x.wait()
    slots[c] = msum[...] + mx[...]
    m_z = [
        remote(slots.at[c], slots.at[c], ms.at[s], mr.at[s], {CTX: me.ahead(s)}) for s in range(1, zn)
    ]
    for s in range(1, zn):
        over_z[s - 1].wait()
        src = me.behind(s)
        done.append(
            remote(ot.at[:, src, t], ot.at[:, src, t], fs.at[s], fr.at[s], {TP: me.t_x})
        )
    for copy in m_z:
        copy.wait()
    value = slots[0]
    for z in range(1, zn):
        value = value + slots[z]
    gsum[me.d] = value
    m_c = remote(gsum.at[me.d], gsum.at[me.d], ms.at[zn], mr.at[zn], {DP: me.d_core})
    m_c.wait()
    pair = gsum.at[pl.ds(me.y * 2, 2)]
    m_y = remote(pair, pair, ms.at[zn + 1], mr.at[zn + 1], {DP: me.d_y})
    m_y.wait()
    for copy in done:
        copy.wait()


def finish(zn, sizes, ai, at_, x_rows, rgrad, out, sums, gains, mod):
    total, dim = rgrad.shape
    n_img, n_txt = sizes
    return call(
        functools.partial(finish_kernel, zn, sizes),
        3,
        [HBM] * 2 + [VMEM] * 6,
        [
            (shaped((2, 2, n_img, dim), BF), HBM),
            (shaped((2, zn, 2, n_txt, dim), BF), HBM),
            (shaped((4, 16, dim), F32), VMEM),
        ],
        sum_scratch(1, zn, total, dim)
        + [
            pltpu.VMEM((2, total, dim), BF),
            pltpu.VMEM((16, dim), F32),
            pltpu.VMEM((16, dim), F32),
            pltpu.VMEM((zn, 16, dim), F32),
            DMA((2,)), DMA((2,)), DMA((zn,)), DMA((zn,)), DMA((zn,)), DMA((zn,)), DMA((2,)),
            DMA((zn + 2,)), DMA((zn + 2,)),
        ],
        (ai, at_, x_rows, rgrad, out, sums, gains, mod),
    )


def return_kernel(
    zn, da, du, dd, ra, ru, rd, own, crecv, part, yrecv,
    loc, cs, cr, ys, yr, zs, zr, ls,
):
    me = Place(zn)
    me.greet()
    y, k = me.y, me.k
    c = me.c
    grads, outs = (da, du, dd), (ra, ru, rd)
    order = [5, 4, 3, 2, 1, 0]
    rows = own.shape[3]
    first = {}
    for chunk in order:
        kind, st = divmod(chunk, 2)
        g = grads[kind]
        group = []
        for j, yy in enumerate((1 - y, y)):
            theirs = g.at[st, pl.ds((yy * 2 + 1 - k) * zn, zn)]
            mine = g.at[st, pl.ds((yy * 2 + k) * zn, zn)]
            group.append(
                (
                    remote(theirs, crecv.at[chunk, j], cs.at[chunk, j], cr.at[chunk, j], {DP: me.d_core}),
                    local(mine, own.at[chunk, j], loc.at[chunk, j]),
                )
            )
        first[chunk] = group
    second = {}

    def add(dst, one, two):
        @pl.loop(0, zn)
        def _(z):
            @pl.loop(0, rows // CHUNK)
            def _(i):
                at = pl.ds(pl.multiple_of(i * CHUNK, CHUNK), CHUNK)
                dst[z, at] = (one[z, at].astype(F32) + two[z, at].astype(F32)).astype(BF)

    for chunk in order:
        for j in range(2):
            for copy in first[chunk][j]:
                copy.wait()
            add(part.at[chunk, j], own.at[chunk, j], crecv.at[chunk, j])
            if j == 0:
                second[chunk] = remote(
                    part.at[chunk, 0], yrecv.at[chunk], ys.at[chunk], yr.at[chunk], {DP: me.d_y}
                )
    last = []
    for chunk in order:
        kind, st = divmod(chunk, 2)
        second[chunk].wait()
        add(own.at[chunk, 0], part.at[chunk, 1], yrecv.at[chunk])
        for s in range(1, zn):
            last.append(
                remote(
                    own.at[chunk, 0, me.ahead(s)],
                    outs[kind].at[c, st],
                    zs.at[chunk, s],
                    zr.at[chunk, s],
                    {CTX: me.ahead(s)},
                )
            )
        last.append(local(own.at[chunk, 0, c], outs[kind].at[c, st], ls.at[chunk]))
    for copy in last:
        copy.wait()


def give_back(zn, da, du, dd):
    rows, width = da.shape[2:]
    shape = shaped((zn, 2, rows, width), BF)
    return call(
        functools.partial(return_kernel, zn),
        4,
        [HBM] * 3,
        [(shape, HBM)] * 3,
        [
            pltpu.VMEM((6, 2, zn, rows, width), BF),
            pltpu.VMEM((6, 2, zn, rows, width), BF),
            pltpu.VMEM((6, 2, zn, rows, width), BF),
            pltpu.VMEM((6, zn, rows, width), BF),
            DMA((6, 2)), DMA((6, 2)), DMA((6, 2)), DMA((6,)), DMA((6,)),
            DMA((6, zn)), DMA((6, zn)), DMA((6,)),
        ],
        (da, du, dd),
    )


def dot(one, two, dims):
    return lax.dot_general(one, two, ((dims[:1], dims[1:]), ((), ())), preferred_element_type=F32)


def split_body(
    img_in, txt_in, cond, mod_weight, qkv_weight, out_weight, up_weight, down_weight, norm_gain,
    cot_img, cot_txt, mod_moment, qkv_moment, out_moment, up_moment, down_moment, gain_moment,
    mod_second, qkv_second, out_second, up_second, down_second, gain_second,
):
    zn = lax.axis_size(CTX)
    dim = img_in.shape[2]
    img_dev, txt_len = img_in.shape[1], txt_in.shape[1]
    n_img = img_dev // 2
    n_txt = -(-txt_len // (2 * zn * CHUNK)) * CHUNK
    sizes = (n_img, n_txt)
    txt_pad = n_txt * 2 * zn
    img_all = img_dev * zn
    head_dim = norm_gain.shape[-1]
    rows = qkv_weight.shape[2]
    col = qkv_weight.shape[4] // zn
    heads = col // head_dim
    ff = up_weight.shape[3] // zn
    scale_factor = head_dim ** (-0.5)
    c, t = lax.axis_index(CTX), lax.axis_index(TP)
    seq = lax.axis_index(DP)
    n_seq = lax.axis_size(DP)

    cond_act = jax.nn.silu(cond.astype(F32)).astype(BF)
    mod_part = product("sm,tmkc->stkc", cond_act, mod_weight[0].astype(BF))
    mod_part = mod_part.reshape(n_seq, -1, 128)

    qkv_low = qkv_weight[0].astype(BF).reshape(2, rows, 3, zn, col)
    qkv_low = jnp.transpose(qkv_low, (3, 0, 1, 2, 4)).reshape(zn, 2, rows, 3 * col)
    out_low = jnp.transpose(out_weight[0].astype(BF).reshape(2, zn, col, rows), (1, 0, 3, 2))
    wa = jnp.concatenate([qkv_low, out_low], axis=3)
    wu = jnp.transpose(up_weight[0].astype(BF).reshape(2, rows, zn, ff), (2, 0, 1, 3))
    wd = jnp.transpose(down_weight[0].astype(BF).reshape(2, zn, ff, rows), (1, 0, 3, 2))

    cot_rows_txt = jnp.pad(cot_txt[0], ((0, txt_pad - txt_len), (0, 0)))
    txt_rows = jnp.pad(txt_in[0], ((0, txt_pad - txt_len), (0, 0)))
    ga, gu, gd, xo, co, mod = spread(
        zn, wa, wu, wd, img_in.reshape(2, n_img, dim), cot_img.reshape(2, n_img, dim), mod_part
    )
    wide = 3 * col + col
    ga = ga.reshape(2, -1, wide)
    gu = gu.reshape(2, -1, ff)
    gd = gd.reshape(2, -1, ff)
    qkv_full = [ga[st, :, : 3 * col] for st in range(2)]
    out_full = [ga[st, :, 3 * col :] for st in range(2)]
    mod = mod.reshape(12, dim)
    mods = [[mod[st * 6 + which][None, :] for which in range(6)] for st in range(2)]

    def own_rows(img, txt):
        one = lax.dynamic_slice_in_dim(img, t * n_img, n_img, 0)
        two = lax.dynamic_slice_in_dim(txt, (c * 2 + t) * n_txt, n_txt, 0)
        return jnp.concatenate([one, two], axis=0)

    x_rows = own_rows(img_in[0], txt_rows)
    cot_rows = own_rows(cot_img[0], cot_rows_txt)
    tokens = [xo.reshape(img_all, dim), txt_rows]
    cots = [co.reshape(img_all, dim), cot_rows_txt]

    hidden, packed = [], []
    for st in range(2):
        normed, _ = layer_norm(tokens[st].astype(F32))
        hidden.append((normed * (1.0 + mods[st][1]) + mods[st][0]).astype(BF))
        packed.append(dot(hidden[st], qkv_full[st], (1, 0)))
    lengths = (img_all, txt_pad)
    packs = [p.reshape(n, 3, heads, head_dim) for p, n in zip(packed, lengths)]
    q_norm = [rms_norm(p[:, 0]) for p in packs]
    k_norm = [rms_norm(p[:, 1]) for p in packs]
    gains = norm_gain[0]

    def by_head(pair):
        return jnp.transpose(jnp.concatenate(pair, axis=0), (1, 0, 2))

    queries = by_head([(q_norm[st][0] * gains[st, 0]).astype(BF) for st in range(2)])
    keys = by_head([(k_norm[st][0] * gains[st, 1]).astype(BF) for st in range(2)])
    values = by_head([packs[st][:, 2].astype(BF) for st in range(2)])
    live = jnp.arange(img_all + txt_pad) < img_all + txt_len
    scores = product("hqd,hkd->hqk", queries, keys) * scale_factor
    scores = jnp.where(live[None, None, :], scores, -1e30)
    peak = jnp.max(scores, axis=-1, keepdims=True)
    log_total = peak + jnp.log(jnp.sum(jnp.exp(scores - peak), axis=-1, keepdims=True))
    probs = jnp.exp(scores - log_total)
    probs_low = probs.astype(BF)
    attended = product("hqk,hkd->hqd", probs_low, values)
    flat = jnp.transpose(attended.astype(BF), (1, 0, 2)).reshape(-1, col)
    flats = [flat[:img_all], flat[img_all:]]

    def blocks(img, txt):
        return img.reshape(zn, 2, n_img, dim), txt.reshape(zn, 2, n_txt, dim)

    proj = [dot(flats[st], out_full[st], (1, 1)).astype(BF) for st in range(2)]
    hi, ht, resid, proj_rows = middle(zn, sizes, *blocks(*proj), x_rows, mod)

    hidden_m = [hi.reshape(img_all, dim), ht.reshape(txt_pad, dim)]
    mlp_out, mlp_in, du, dd = [], [], [], []
    for st in range(2):
        pre_act = dot(hidden_m[st], gu[st], (1, 0))
        activated, pull = jax.vjp(gelu_tanh, pre_act)
        activated = activated.astype(BF)
        mlp_out.append(dot(activated, gd[st], (1, 1)).astype(BF))
        branch = (cots[st].astype(F32) * mods[st][5]).astype(BF)
        pre_grad = pull(dot(branch, gd[st], (1, 0)))[0].astype(BF)
        mlp_in.append(dot(pre_grad, gu[st], (1, 1)).astype(BF))
        dd.append(dot(branch, activated, (0, 0)).astype(BF))
        du.append(dot(hidden_m[st], pre_grad, (0, 0)).astype(BF))
    bi, bt, out_rows, rgrad, sums = turn(
        zn, sizes, *blocks(*mlp_in), *blocks(*mlp_out), resid, proj_rows, cot_rows, mod
    )

    branch_a = [bi.reshape(img_all, dim), bt.reshape(txt_pad, dim)]
    att_grad = jnp.concatenate([dot(branch_a[st], out_full[st], (1, 0)) for st in range(2)], axis=0)
    att_grad = jnp.transpose(att_grad.astype(BF).reshape(-1, heads, head_dim), (1, 0, 2))
    delta = jnp.sum(att_grad.astype(F32) * attended, axis=-1, keepdims=True)
    prob_grad = product("hqd,hkd->hqk", att_grad, values)
    score_grad = (probs * (prob_grad - delta) * scale_factor).astype(BF)
    query_grad = jnp.transpose(product("hqk,hkd->hqd", score_grad, keys), (1, 0, 2))
    key_grad = jnp.transpose(product("hqk,hqd->hkd", score_grad, queries), (1, 0, 2))
    value_grad = jnp.transpose(product("hqk,hqd->hkd", probs_low, att_grad), (1, 0, 2))
    gain_lines, input_part, da = [], [], []
    for st in range(2):
        part = slice(0, img_all) if st == 0 else slice(img_all, None)
        q_grad, k_grad = query_grad[part], key_grad[part]
        gain_lines.append(jnp.sum(q_grad * q_norm[st][0], axis=(0, 1)))
        gain_lines.append(jnp.sum(k_grad * k_norm[st][0], axis=(0, 1)))
        q_raw = rms_back(q_grad * gains[st, 0], *q_norm[st])
        k_raw = rms_back(k_grad * gains[st, 1], *k_norm[st])
        packed_grad = jnp.stack([q_raw, k_raw, value_grad[part]], axis=1)
        packed_grad = packed_grad.reshape(-1, 3 * col).astype(BF)
        input_part.append(dot(packed_grad, qkv_full[st], (1, 1)).astype(BF))
        d_qkv = dot(hidden[st], packed_grad, (0, 0)).astype(BF)
        d_out = dot(branch_a[st], flats[st], (0, 0)).astype(BF)
        da.append(jnp.concatenate([d_qkv, d_out], axis=1))
    gain_row = jnp.pad(jnp.concatenate(gain_lines), (0, dim - 4 * head_dim))[None, :]
    oi, ot, gsum = finish(zn, sizes, *blocks(*input_part), x_rows, rgrad, out_rows, sums, gain_row, mod)
    img_out, img_grad = oi[0].reshape(1, img_dev, dim), oi[1].reshape(1, img_dev, dim)
    txt_out = ot[0].reshape(1, txt_pad, dim)[:, :txt_len]
    txt_grad = ot[1].reshape(1, txt_pad, dim)[:, :txt_len]

    def stacked(pair):
        return jnp.stack(pair).reshape(2, n_seq * zn, rows, -1)

    ra, ru, rd = give_back(zn, stacked(da), stacked(du), stacked(dd))
    qkv_grad = ra[..., : 3 * col].reshape(zn, 2, rows, 3, col)
    qkv_grad = jnp.transpose(qkv_grad, (1, 2, 3, 0, 4)).reshape(qkv_weight.shape).astype(F32)
    out_grad = jnp.transpose(ra[..., 3 * col :], (1, 0, 3, 2)).reshape(out_weight.shape).astype(F32)
    up_grad = jnp.transpose(ru, (1, 2, 0, 3)).reshape(up_weight.shape).astype(F32)
    down_grad = jnp.transpose(rd, (1, 0, 3, 2)).reshape(down_weight.shape).astype(F32)

    gain_grad = jnp.sum(gsum[:, 12, : 4 * head_dim], axis=0).reshape(norm_gain.shape)
    mod_rows = gsum[:, :12].reshape(n_seq, 2, 1, 6, dim)
    cond_col = cond_act.astype(F32)[:, None, :, None, None]
    mod_grad = jnp.sum(cond_col * mod_rows, axis=0)[None]

    results = [img_out, txt_out, img_grad, txt_grad]
    for weight, moment, second, grad in (
        (mod_weight, mod_moment, mod_second, mod_grad),
        (qkv_weight, qkv_moment, qkv_second, qkv_grad),
        (out_weight, out_moment, out_second, out_grad),
        (up_weight, up_moment, up_second, up_grad),
        (down_weight, down_moment, down_second, down_grad),
        (norm_gain, gain_moment, gain_second, gain_grad),
    ):
        results.append(grad)
        results.extend(adam_step(weight, moment, second, grad))
    return tuple(results)


def fits_split(mesh, args):
    dp, zn, tp = (mesh.shape[axis] for axis in ALL)
    img, txt, gain, qkv, up = args[0], args[1], args[8], args[4], args[6]
    heads = qkv.shape[4] // gain.shape[-1]
    return (
        dp == 4
        and tp == 2
        and zn > 1
        and qkv.shape[0] == 1
        and img.shape[0] == dp
        and heads % (tp * zn) == 0
        and (4 * qkv.shape[4] // (tp * zn)) % 128 == 0
        and (up.shape[3] // (tp * zn)) % 128 == 0
        and img.shape[1] % (zn * 2 * CHUNK) == 0
        and img.shape[2] % 128 == 0
        and img.shape[2] % (dp * zn * CHUNK) == 0
        and 4 * gain.shape[-1] <= img.shape[2]
    )


def solution(mesh):
    tokens = [P(DP, CTX, None), P(DP, None, None)]
    mod_spec = P(None, None, ALL, None, None)
    qkv_spec = P(None, None, ROWS, None, TP)
    out_spec = P(None, None, TP, ROWS)
    up_spec = P(None, None, ROWS, TP)
    weights = [mod_spec, qkv_spec, out_spec, up_spec, out_spec, P()]
    in_specs = tuple(tokens + [P(None, ALL)] + weights + tokens + weights + weights)
    out_specs = tuple(tokens + tokens + [spec for spec in weights for _ in range(4)])

    def step(*args):
        body = split_body if fits_split(mesh, args) else gathered_body
        return jax.shard_map(
            body, mesh=mesh, in_specs=in_specs, out_specs=out_specs, check_vma=False
        )(*args)

    return step
```

```python
import functools
from types import SimpleNamespace as NS

import jax
import jax.numpy as jnp
from jax import lax
from jax.experimental import pallas as pl
from jax.experimental.pallas import tpu as pltpu
from jax.sharding import PartitionSpec as P

DP, CTX, TP = "dp", "ctx", "tp"
ROWS = (DP, CTX)
ALL = (DP, CTX, TP)

norm_eps = 1e-06
learn_rate = 0.004
beta_one = 0.9
beta_two = 0.999
adam_eps = 1e-08
decay_rate = 0.1
corr_one = 1.0 - beta_one**3
corr_two = 1.0 - beta_two**3

BF = jnp.bfloat16
F32 = jnp.float32


def product(pattern, former, latter):
    return jnp.einsum(pattern, former, latter, preferred_element_type=jnp.float32)


def layer_norm(values):
    center = values - jnp.mean(values, axis=-1, keepdims=True)
    spread = lax.rsqrt(jnp.mean(center * center, axis=-1, keepdims=True) + norm_eps)
    return (center * spread, spread)


def norm_back(incoming, normed, spread):
    return spread * (
        incoming
        - jnp.mean(incoming, axis=-1, keepdims=True)
        - normed * jnp.mean(incoming * normed, axis=-1, keepdims=True)
    )


def rms_norm(raw_rows):
    factor = lax.rsqrt(jnp.mean(raw_rows * raw_rows, axis=-1, keepdims=True) + norm_eps)
    return (raw_rows * factor, factor)


def rms_back(incoming, normed, factor):
    return factor * (incoming - normed * jnp.mean(incoming * normed, axis=-1, keepdims=True))


def gelu_tanh(values):
    return jax.nn.gelu(values, approximate=True)


def adam_step(weight, moment, second, gradient):
    new_moment = beta_one * moment + (1.0 - beta_one) * gradient
    new_second = beta_two * second + (1.0 - beta_two) * gradient * gradient
    update = (
        new_moment / corr_one / (jnp.sqrt(new_second / corr_two) + adam_eps) + decay_rate * weight
    )
    return (weight - learn_rate * update, new_moment, new_second)


def modulate(normed, shift_vec, scale_vec):
    return (normed * (1.0 + scale_vec[:, None, :]) + shift_vec[:, None, :]).astype(jnp.bfloat16)


def stream_front(inputs, modulation, qkv_part, gain_pair):
    values = inputs.astype(jnp.float32)
    normed, spread = layer_norm(values)
    hidden = modulate(normed, modulation[:, 0], modulation[:, 1])
    packed = product("btd,dkc->btkc", hidden, qkv_part)
    packed = packed.reshape(packed.shape[0], packed.shape[1], 3, -1, gain_pair.shape[-1])
    q_hat, q_factor = rms_norm(packed[:, :, 0])
    k_hat, k_factor = rms_norm(packed[:, :, 1])
    return NS(        values=values,
        normed=normed,
        spread=spread,
        hidden=hidden,
        q_hat=q_hat,
        q_factor=q_factor,
        k_hat=k_hat,
        k_factor=k_factor,
        queries=(q_hat * gain_pair[0]).astype(jnp.bfloat16),
        key_rows=(k_hat * gain_pair[1]).astype(jnp.bfloat16),
        value_rows=packed[:, :, 2].astype(jnp.bfloat16),)


def mlp_front(resid, modulation, up_part):
    normed, spread = layer_norm(resid)
    hidden = modulate(normed, modulation[:, 3], modulation[:, 4])
    pre_act = product("btd,df->btf", hidden, up_part)
    activated = gelu_tanh(pre_act).astype(jnp.bfloat16)
    return NS(        normed=normed,
        spread=spread,
        hidden=hidden,
        pre_act=pre_act,
        activated=activated,)


def attend(query_all, key_all, value_all, scale_factor):
    scores = product("bqhd,bkhd->bhqk", query_all, key_all) * scale_factor
    row_peak = jnp.max(scores, axis=-1, keepdims=True)
    log_total = row_peak + jnp.log(jnp.sum(jnp.exp(scores - row_peak), axis=-1, keepdims=True))
    attn_probs = jnp.exp(scores - log_total).astype(jnp.bfloat16)
    attended = product("bhqk,bkhd->bqhd", attn_probs, value_all)
    return (attended, log_total)


def attend_back(
    grad_att, query_all, key_all, value_all, attended, log_total, scale_factor, split_at
):
    row_delta = jnp.sum(grad_att.astype(jnp.float32) * attended, axis=-1)
    scores = product("bqhd,bkhd->bhqk", query_all, key_all) * scale_factor
    attn_probs = jnp.exp(scores - log_total)
    prob_grad = product("bqhd,bkhd->bhqk", grad_att, value_all)
    score_grad = (
        attn_probs * (prob_grad - jnp.transpose(row_delta, (0, 2, 1))[..., None]) * scale_factor
    ).astype(jnp.bfloat16)
    probs_low = attn_probs.astype(jnp.bfloat16)
    query_grad = product("bhqk,bkhd->bqhd", score_grad, key_all)
    key_first = product("bhqk,bqhd->bkhd", score_grad[:, :, :split_at], query_all[:, :split_at])
    key_second = product("bhqk,bqhd->bkhd", score_grad[:, :, split_at:], query_all[:, split_at:])
    value_first = product("bhqk,bqhd->bkhd", probs_low[:, :, :split_at], grad_att[:, :split_at])
    value_second = product("bhqk,bqhd->bkhd", probs_low[:, :, split_at:], grad_att[:, split_at:])
    return (query_grad, key_first, key_second, value_first, value_second)


def mlp_back(grad_out, modulation, mlp_parts, down_out, up_part, down_part):
    gate_two = jnp.sum(grad_out * down_out, axis=1)
    branch = (grad_out * modulation[:, 5][:, None, :]).astype(jnp.bfloat16)
    act_grad = product("btd,fd->btf", branch, down_part)
    down_term = product("btf,btd->fd", mlp_parts.activated, branch)
    pre_grad = jax.vjp(gelu_tanh, mlp_parts.pre_act)[1](act_grad)[0].astype(jnp.bfloat16)
    up_term = product("btd,btf->df", mlp_parts.hidden, pre_grad)
    hidden_part = product("btf,df->btd", pre_grad, up_part)
    return (gate_two, down_term, up_term, hidden_part)


def norm_branch_back(hidden_grad, normed, spread, scale_vec, residual_grad):
    shift_grad = jnp.sum(hidden_grad, axis=1)
    scale_grad = jnp.sum(hidden_grad * normed, axis=1)
    total = residual_grad + norm_back(hidden_grad * (1.0 + scale_vec[:, None, :]), normed, spread)
    return (shift_grad, scale_grad, total)


def attention_branch_back(resid_grad, modulation, proj, flat_rows, out_part):
    gate_one = jnp.sum(resid_grad * proj, axis=1)
    branch = (resid_grad * modulation[:, 2][:, None, :]).astype(jnp.bfloat16)
    att_grad = product("btd,cd->btc", branch, out_part)
    out_term = product("btc,btd->cd", flat_rows, branch)
    return (gate_one, att_grad, out_term)


def head_back(query_grad, key_grad, value_grad, front, gain_pair):
    gain_term = jnp.stack(
        [
            jnp.sum(query_grad * front.q_hat, axis=(0, 1, 2)),
            jnp.sum(key_grad * front.k_hat, axis=(0, 1, 2)),
        ]
    )
    q_raw = rms_back(query_grad * gain_pair[0], front.q_hat, front.q_factor)
    k_raw = rms_back(key_grad * gain_pair[1], front.k_hat, front.k_factor)
    packed = jnp.stack([q_raw, k_raw, value_grad], axis=2)
    packed = packed.reshape(packed.shape[0], packed.shape[1], 3, -1).astype(jnp.bfloat16)
    return (gain_term, packed)


def gathered_body(
    img_in,
    txt_in,
    cond,
    mod_weight,
    qkv_weight,
    out_weight,
    up_weight,
    down_weight,
    norm_gain,
    cot_img,
    cot_txt,
    mod_moment,
    qkv_moment,
    out_moment,
    up_moment,
    down_moment,
    gain_moment,
    mod_second,
    qkv_second,
    out_second,
    up_second,
    down_second,
    gain_second,
):
    ctx_count = lax.axis_size(CTX)
    tp_count = lax.axis_size(TP)
    seq_dev = img_in.shape[0]
    img_dev = img_in.shape[1]
    txt_rows = txt_in.shape[1]
    img_total = img_dev * ctx_count
    layer_count = qkv_weight.shape[0]
    head_dim = norm_gain.shape[-1]
    scale_factor = head_dim ** (-0.5)
    seq_start = lax.axis_index(DP) * seq_dev
    ctx_start = lax.axis_index(CTX) * img_dev
    cond_act = jax.nn.silu(cond.astype(jnp.float32)).astype(jnp.bfloat16)
    mod_part = product("sm,ltmkc->ltskc", cond_act, mod_weight.astype(jnp.bfloat16))
    all_mod = lax.psum(mod_part, ALL)
    own_mod = lax.dynamic_slice_in_dim(all_mod, seq_start, seq_dev, 2)

    def gather_weights(layer_id):
        return (
            lax.all_gather(
                qkv_weight[layer_id].astype(jnp.bfloat16), ROWS, axis=1, tiled=True
            ),
            lax.all_gather(
                out_weight[layer_id].astype(jnp.bfloat16), ROWS, axis=2, tiled=True
            ),
            lax.all_gather(
                up_weight[layer_id].astype(jnp.bfloat16), ROWS, axis=1, tiled=True
            ),
            lax.all_gather(
                down_weight[layer_id].astype(jnp.bfloat16), ROWS, axis=2, tiled=True
            ),
        )

    def joined_keys(front_pair):
        remote_keys, remote_values = (
            lax.all_gather(front_pair[0].key_rows, CTX, axis=1, tiled=True),
            lax.all_gather(front_pair[0].value_rows, CTX, axis=1, tiled=True),
        )
        key_all = jnp.concatenate([remote_keys, front_pair[1].key_rows], axis=1)
        value_all = jnp.concatenate([remote_values, front_pair[1].value_rows], axis=1)
        return (key_all, value_all)

    streams = [img_in, txt_in]
    layer_id = 0
    full_qkv, full_out, full_up, full_down = gather_weights(layer_id)
    mod_pair = [own_mod[layer_id, 0], own_mod[layer_id, 1]]
    front_pair = [
        stream_front(
            streams[stream_id],
            mod_pair[stream_id],
            full_qkv[stream_id],
            norm_gain[layer_id, stream_id],
        )
        for stream_id in range(2)
    ]
    key_all, value_all = joined_keys(front_pair)
    query_all = jnp.concatenate([front_pair[0].queries, front_pair[1].queries], axis=1)
    attended, log_total = attend(query_all, key_all, value_all, scale_factor)
    attended_low = attended.astype(jnp.bfloat16)
    flat_pair = [
        attended_low[:, :img_dev].reshape(seq_dev, img_dev, -1),
        attended_low[:, img_dev:].reshape(seq_dev, txt_rows, -1),
    ]
    proj_img = lax.psum(
        product("btc,cd->btd", flat_pair[0], full_out[0]).astype(jnp.bfloat16), TP
    ).astype(jnp.float32)
    proj_txt = lax.psum(
        product("btc,cd->btd", flat_pair[1], full_out[1]).astype(jnp.bfloat16), TP
    ).astype(jnp.float32)
    proj_pair = [proj_img, proj_txt]
    resid_pair = [
        front_pair[stream_id].values
        + mod_pair[stream_id][:, 2][:, None, :] * proj_pair[stream_id]
        for stream_id in range(2)
    ]
    mlp_pair = [
        mlp_front(resid_pair[stream_id], mod_pair[stream_id], full_up[stream_id])
        for stream_id in range(2)
    ]
    down_img = lax.psum(
        product("btf,fd->btd", mlp_pair[0].activated, full_down[0]).astype(jnp.bfloat16), TP
    ).astype(jnp.float32)
    down_txt = lax.psum(
        product("btf,fd->btd", mlp_pair[1].activated, full_down[1]).astype(jnp.bfloat16), TP
    ).astype(jnp.float32)
    down_pair = [down_img, down_txt]
    streams = [
        resid_pair[stream_id] + mod_pair[stream_id][:, 5][:, None, :] * down_pair[stream_id]
        for stream_id in range(2)
    ]
    stored = [
        NS(            weights=(full_qkv, full_out, full_up, full_down),
            front=front_pair,
            key_all=key_all,
            value_all=value_all,
            query_all=query_all,
            attended=attended,
            log_total=log_total,
            flat=flat_pair,
            proj=proj_pair,
            mlp=mlp_pair,
            down=down_pair,)
    ]
    grads = [cot_img.astype(jnp.float32), cot_txt.astype(jnp.float32)]
    mod_terms = [None] * layer_count
    gain_terms = [None] * layer_count
    owned_grads = [None] * layer_count
    for layer_id in reversed(range(layer_count)):
        saved = stored[layer_id]
        mod_pair = [own_mod[layer_id, 0], own_mod[layer_id, 1]]
        front_pair = saved.front
        full_qkv, full_out, full_up, full_down = gather_weights(layer_id)
        key_all, value_all = joined_keys(front_pair)
        mlp_parts = [
            mlp_back(
                grads[stream_id],
                mod_pair[stream_id],
                saved.mlp[stream_id],
                saved.down[stream_id],
                full_up[stream_id],
                full_down[stream_id],
            )
            for stream_id in range(2)
        ]
        hidden_img, hidden_txt = (
            lax.psum(mlp_parts[0][3].astype(jnp.bfloat16), TP).astype(jnp.float32),
            lax.psum(mlp_parts[1][3].astype(jnp.bfloat16), TP).astype(jnp.float32),
        )
        hidden_pair = [hidden_img, hidden_txt]
        mlp_norm = [
            norm_branch_back(
                hidden_pair[stream_id],
                saved.mlp[stream_id].normed,
                saved.mlp[stream_id].spread,
                mod_pair[stream_id][:, 4],
                grads[stream_id],
            )
            for stream_id in range(2)
        ]
        attn_parts = [
            attention_branch_back(
                mlp_norm[stream_id][2],
                mod_pair[stream_id],
                saved.proj[stream_id],
                saved.flat[stream_id],
                full_out[stream_id],
            )
            for stream_id in range(2)
        ]
        grad_att = jnp.concatenate(
            [
                attn_parts[0][1].reshape(seq_dev, img_dev, -1, head_dim),
                attn_parts[1][1].reshape(seq_dev, txt_rows, -1, head_dim),
            ],
            axis=1,
        ).astype(jnp.bfloat16)
        query_grad, key_first, key_second, value_first, value_second = attend_back(
            grad_att,
            saved.query_all,
            key_all,
            value_all,
            saved.attended,
            saved.log_total,
            scale_factor,
            img_dev,
        )
        key_img_sum, value_img_sum = (
            lax.psum_scatter(
                key_first[:, :img_total].astype(jnp.bfloat16),
                CTX,
                scatter_dimension=1,
                tiled=True,
            ).astype(jnp.float32),
            lax.psum_scatter(
                value_first[:, :img_total].astype(jnp.bfloat16),
                CTX,
                scatter_dimension=1,
                tiled=True,
            ).astype(jnp.float32),
        )
        key_txt_sum, value_txt_sum = (
            lax.psum(key_first[:, img_total:].astype(jnp.bfloat16), CTX).astype(jnp.float32),
            lax.psum(value_first[:, img_total:].astype(jnp.bfloat16), CTX).astype(jnp.float32),
        )
        key_pair = [
            key_img_sum
            + lax.dynamic_slice_in_dim(key_second[:, :img_total], ctx_start, img_dev, 1),
            key_txt_sum + key_second[:, img_total:],
        ]
        value_pair = [
            value_img_sum
            + lax.dynamic_slice_in_dim(value_second[:, :img_total], ctx_start, img_dev, 1),
            value_txt_sum + value_second[:, img_total:],
        ]
        query_pair = [query_grad[:, :img_dev], query_grad[:, img_dev:]]
        head_parts = [
            head_back(
                query_pair[stream_id],
                key_pair[stream_id],
                value_pair[stream_id],
                front_pair[stream_id],
                norm_gain[layer_id, stream_id],
            )
            for stream_id in range(2)
        ]
        input_img, input_txt = (
            lax.psum(
                product("btkc,dkc->btd", head_parts[0][1], full_qkv[0]).astype(jnp.bfloat16), TP
            ).astype(jnp.float32),
            lax.psum(
                product("btkc,dkc->btd", head_parts[1][1], full_qkv[1]).astype(jnp.bfloat16), TP
            ).astype(jnp.float32),
        )
        input_pair = [input_img, input_txt]
        attn_norm = [
            norm_branch_back(
                input_pair[stream_id],
                front_pair[stream_id].normed,
                front_pair[stream_id].spread,
                mod_pair[stream_id][:, 1],
                mlp_norm[stream_id][2],
            )
            for stream_id in range(2)
        ]
        grads = [attn_norm[stream_id][2] for stream_id in range(2)]
        mod_rows = [
            jnp.stack(
                [
                    attn_norm[stream_id][0],
                    attn_norm[stream_id][1],
                    attn_parts[stream_id][0],
                    mlp_norm[stream_id][0],
                    mlp_norm[stream_id][1],
                    mlp_parts[stream_id][0],
                ],
                axis=1,
            )
            for stream_id in range(2)
        ]
        mod_terms[layer_id] = jnp.stack([mod_rows[0], mod_rows[1] / ctx_count]) / tp_count
        gain_terms[layer_id] = jnp.stack([head_parts[0][0], head_parts[1][0] / ctx_count])
        qkv_stack = jnp.stack(
            [
                product("btd,btkc->dkc", front_pair[stream_id].hidden, head_parts[stream_id][1])
                for stream_id in range(2)
            ]
        )
        out_stack = jnp.stack([attn_parts[stream_id][2] for stream_id in range(2)])
        up_stack = jnp.stack([mlp_parts[stream_id][2] for stream_id in range(2)])
        down_stack = jnp.stack([mlp_parts[stream_id][1] for stream_id in range(2)])
        qkv_term = jnp.concatenate([qkv_stack[0:1], qkv_stack[1:2] / ctx_count])
        out_term = jnp.concatenate([out_stack[0:1], out_stack[1:2] / ctx_count])
        up_term = jnp.concatenate([up_stack[0:1], up_stack[1:2] / ctx_count])
        down_term = jnp.concatenate([down_stack[0:1], down_stack[1:2] / ctx_count])
        owned = (
            lax.psum_scatter(
                qkv_term.astype(jnp.bfloat16), ROWS, scatter_dimension=1, tiled=True
            ).astype(jnp.float32),
            lax.psum_scatter(
                out_term.astype(jnp.bfloat16), ROWS, scatter_dimension=2, tiled=True
            ).astype(jnp.float32),
            lax.psum_scatter(
                up_term.astype(jnp.bfloat16), ROWS, scatter_dimension=1, tiled=True
            ).astype(jnp.float32),
            lax.psum_scatter(
                down_term.astype(jnp.bfloat16), ROWS, scatter_dimension=2, tiled=True
            ).astype(jnp.float32),
        )
        owned_grads[layer_id] = owned
    mod_local = jnp.stack(mod_terms)
    mod_zero = jnp.zeros(
        (layer_count, 2, seq_dev * lax.axis_size(DP)) + mod_local.shape[3:], jnp.float32
    )
    mod_term = lax.dynamic_update_slice_in_dim(mod_zero, mod_local, seq_start, 2)
    mod_full, gain_grad = lax.psum((mod_term, jnp.stack(gain_terms)), ALL)
    mod_grad = jnp.einsum(
        "sm,ltskc->ltmkc", cond_act.astype(jnp.float32), mod_full, precision=lax.Precision.HIGHEST
    )
    qkv_grad = jnp.stack([owned_grads[0][0]])
    out_grad = jnp.stack([owned_grads[0][1]])
    up_grad = jnp.stack([owned_grads[0][2]])
    down_grad = jnp.stack([owned_grads[0][3]])
    mod_next, mod_moment_next, mod_second_next = adam_step(
        mod_weight, mod_moment, mod_second, mod_grad
    )
    qkv_next, qkv_moment_next, qkv_second_next = adam_step(
        qkv_weight, qkv_moment, qkv_second, qkv_grad
    )
    out_next, out_moment_next, out_second_next = adam_step(
        out_weight, out_moment, out_second, out_grad
    )
    up_next, up_moment_next, up_second_next = adam_step(up_weight, up_moment, up_second, up_grad)
    down_next, down_moment_next, down_second_next = adam_step(
        down_weight, down_moment, down_second, down_grad
    )
    gain_next, gain_moment_next, gain_second_next = adam_step(
        norm_gain, gain_moment, gain_second, gain_grad
    )
    return (
        streams[0].astype(jnp.bfloat16),
        streams[1].astype(jnp.bfloat16),
        grads[0].astype(jnp.bfloat16),
        grads[1].astype(jnp.bfloat16),
        mod_grad,
        mod_next,
        mod_moment_next,
        mod_second_next,
        qkv_grad,
        qkv_next,
        qkv_moment_next,
        qkv_second_next,
        out_grad,
        out_next,
        out_moment_next,
        out_second_next,
        up_grad,
        up_next,
        up_moment_next,
        up_second_next,
        down_grad,
        down_next,
        down_moment_next,
        down_second_next,
        gain_grad,
        gain_next,
        gain_moment_next,
        gain_second_next,
    )


class Place:
    def __init__(self, zn):
        self.zn = zn
        self.d, self.c, self.t = lax.axis_index(DP), lax.axis_index(CTX), lax.axis_index(TP)
        self.y, self.k = self.d // 2, self.d % 2
        self.d_core = self.y * 2 + (1 - self.k)
        self.d_y = (1 - self.y) * 2 + self.k
        self.t_x = 1 - self.t

    def ahead(self, step):
        return (self.c + step) % self.zn

    def behind(self, step):
        return (self.c + self.zn - step) % self.zn

    def greet(self, core=True, y=True, x=True, z=True):
        sem = pltpu.get_barrier_semaphore()
        count = 0
        for wanted, where in ((x, {TP: self.t_x}), (core, {DP: self.d_core}), (y, {DP: self.d_y})):
            if wanted:
                pl.semaphore_signal(sem, inc=1, device_id=where, device_id_type=pl.DeviceIdType.MESH)
                count += 1
        if z:
            for step in range(1, self.zn):
                pl.semaphore_signal(
                    sem, inc=1, device_id={CTX: self.ahead(step)}, device_id_type=pl.DeviceIdType.MESH
                )
                count += 1
        pl.semaphore_wait(sem, count)


def remote(src, dst, send, recv, where):
    copy = pltpu.make_async_remote_copy(
        src_ref=src,
        dst_ref=dst,
        send_sem=send,
        recv_sem=recv,
        device_id=where,
        device_id_type=pl.DeviceIdType.MESH,
    )
    copy.start()
    return copy


def local(src, dst, sem):
    copy = pltpu.make_async_copy(src, dst, sem)
    copy.start()
    return copy


HBM = pl.BlockSpec(memory_space=pl.ANY)
VMEM = pl.BlockSpec(memory_space=pltpu.VMEM)
DMA = pltpu.SemaphoreType.DMA


def call(kernel, ident, ins, outs, scratch, args, flops=0):
    return pl.pallas_call(
        kernel,
        out_shape=[shape for shape, _ in outs],
        in_specs=ins,
        out_specs=[spec for _, spec in outs],
        scratch_shapes=scratch,
        compiler_params=pltpu.CompilerParams(
            collective_id=ident, has_side_effects=True, vmem_limit_bytes=60 * 1024 * 1024
        ),
    )(*args)


def shaped(shape, dtype):
    return jax.ShapeDtypeStruct(shape, dtype)


CHUNK = 8


def sum_start(me, arrays, own, recvx, xs, xr, loc):
    order = list(range(1, me.zn)) + [0]
    copies = {}
    for a, parts in enumerate(arrays):
        for s in order:
            zb = me.ahead(s)
            at = 0
            group = []
            for p, part in enumerate(parts):
                n = part.shape[2]
                group.append(
                    remote(
                        part.at[zb, me.t_x],
                        recvx.at[a, s, pl.ds(at, n)],
                        xs.at[a, s, p],
                        xr.at[a, s, p],
                        {TP: me.t_x},
                    )
                )
                group.append(local(part.at[zb, me.t], own.at[a, s, pl.ds(at, n)], loc.at[a, s, p]))
                at += n
            copies[a, s] = group
    return copies


def sum_x(me, a, copies, own, recvx, sumb, recvz, total, zs, zr):
    rows = own.shape[2]
    out = []
    for s in list(range(1, me.zn)) + [0]:
        for copy in copies[a, s]:
            copy.wait()
        if s:

            @pl.loop(0, rows // CHUNK)
            def _(i):
                at = pl.ds(pl.multiple_of(i * CHUNK, CHUNK), CHUNK)
                sumb[a, s, at] = (own[a, s, at].astype(F32) + recvx[a, s, at].astype(F32)).astype(BF)

            out.append(
                remote(sumb.at[a, s], recvz.at[a, s], zs.at[a, s], zr.at[a, s], {CTX: me.ahead(s)})
            )
        else:

            @pl.loop(0, rows // CHUNK)
            def _(i):
                at = pl.ds(pl.multiple_of(i * CHUNK, CHUNK), CHUNK)
                total[a, at] = own[a, s, at].astype(F32) + recvx[a, s, at].astype(F32)

    return out


def sum_z(me, a, copies, recvz, total):
    for copy in copies:
        copy.wait()
    rows = total.shape[1]

    @pl.loop(0, rows // CHUNK)
    def _(i):
        at = pl.ds(pl.multiple_of(i * CHUNK, CHUNK), CHUNK)
        value = total[a, at]
        for s in range(1, me.zn):
            value = value + recvz[a, s, at].astype(F32)
        total[a, at] = value


def share_start(me, block, outs, sizes, zs, zr, xs, xr, loc):
    copies = []
    at = 0
    for p, (o, n) in enumerate(zip(outs, sizes)):
        src = block.at[pl.ds(at, n)]
        at += n
        dst = o.at[me.c, me.t]
        group = [
            remote(src, dst, zs.at[p, s], zr.at[p, s], {CTX: me.ahead(s)}) for s in range(1, me.zn)
        ]
        group.append(remote(src, dst, xs.at[p, 0], xr.at[p, 0], {TP: me.t_x}))
        group.append(local(src, dst, loc.at[p]))
        copies.append(group)
    return copies


def share_end(me, copies, outs, xs, xr):
    passed = []
    for s in range(1, me.zn):
        src = me.behind(s)
        for p, o in enumerate(outs):
            copies[p][s - 1].wait()
            passed.append(
                remote(o.at[src, me.t], o.at[src, me.t], xs.at[p, s], xr.at[p, s], {TP: me.t_x})
            )
    for group in copies:
        for copy in group[me.zn - 1 :]:
            copy.wait()
    for copy in passed:
        copy.wait()


def row_loops(sizes, fn):
    at = 0
    for stream, n in enumerate(sizes):

        @pl.loop(0, n // CHUNK)
        def _(i, at=at, stream=stream):
            fn(stream, pl.ds(pl.multiple_of(at + i * CHUNK, CHUNK), CHUNK))

        at += n


def line(mod, stream, which):
    return mod[stream * 6 + which][None, :]


def sum_scratch(count, zn, rows, dim):
    return [
        pltpu.VMEM((count, zn, rows, dim), BF),
        pltpu.VMEM((count, zn, rows, dim), BF),
        pltpu.VMEM((count, zn, rows, dim), BF),
        pltpu.VMEM((count, zn, rows, dim), BF),
        pltpu.VMEM((count, rows, dim), F32),
        DMA((count, zn, 2)), DMA((count, zn, 2)), DMA((count, zn, 2)),
        DMA((count, zn)), DMA((count, zn)),
    ]


def share_scratch(zn, rows, dim):
    return [
        pltpu.VMEM((rows, dim), BF),
        DMA((2, zn)), DMA((2, zn)), DMA((2, zn)), DMA((2, zn)), DMA((2,)),
    ]


class PairSum:
    def __init__(self, me, grads, outs, crecv, part, yrecv, cs, cr, ys, yr, ls):
        self.me, self.grads, self.outs = me, grads, outs
        self.crecv, self.part, self.yrecv = crecv, part, yrecv
        self.cs, self.cr, self.ys, self.yr, self.ls = cs, cr, ys, yr, ls
        self.chunks = [(kind, st) for kind in range(grads.shape[0]) for st in range(2)]
        self.first, self.second, self.last = {}, {}, []
        self.span = yrecv.shape[1]

    def rows(self, y, core, more=0, n=None):
        first = (y * 2 + core) * self.span + more
        return pl.ds(pl.multiple_of(first, 16), n or self.span)

    def start(self, at):
        me = self.me
        kind, st = self.chunks[at]
        for j, yy in enumerate((1 - me.y, me.y)):
            self.first[at, j] = remote(
                self.grads.at[kind, st, self.rows(yy, 1 - me.k)],
                self.crecv.at[at, j],
                self.cs.at[at, j],
                self.cr.at[at, j],
                {DP: me.d_core},
            )

    def across(self, at):
        me = self.me
        kind, st = self.chunks[at]
        for j, yy in enumerate((1 - me.y, me.y)):
            self.first[at, j].wait()

            @pl.loop(0, self.span // 16)
            def _(i, j=j, yy=yy):
                to = pl.ds(pl.multiple_of(i * 16, 16), 16)
                mine = self.grads[kind, st, self.rows(yy, me.k, i * 16, 16)]
                self.part[at, j, to] = (mine.astype(F32) + self.crecv[at, j, to].astype(F32)).astype(BF)

            if j == 0:
                self.second[at] = remote(
                    self.part.at[at, 0], self.yrecv.at[at], self.ys.at[at], self.yr.at[at], {DP: me.d_y}
                )

    def end(self):
        me = self.me
        each = self.span // me.zn
        for at, (kind, st) in enumerate(self.chunks):
            self.second[at].wait()

            @pl.loop(0, self.span // 16)
            def _(i, at=at):
                to = pl.ds(pl.multiple_of(i * 16, 16), 16)
                self.crecv[at, 0, to] = (
                    self.part[at, 1, to].astype(F32) + self.yrecv[at, to].astype(F32)
                ).astype(BF)

            for s in range(me.zn):
                rows = pl.ds(pl.multiple_of(me.ahead(s) * each, 16), each)
                self.last.append(
                    local(self.crecv.at[at, 0, rows], self.outs[s].at[kind, st], self.ls.at[at, s])
                )
        for copy in self.last:
            copy.wait()


def pair_scratch(kinds, zn, rows, width):
    n = 2 * kinds
    return [
        pltpu.VMEM((n, 2, zn * rows, width), BF),
        pltpu.VMEM((n, 2, zn * rows, width), BF),
        pltpu.VMEM((n, zn * rows, width), BF),
        DMA((n, 2)), DMA((n, 2)), DMA((n,)), DMA((n,)), DMA((n, zn)),
    ]


def pair_outs(kinds, zn, rows, width):
    return [(shaped((kinds, 2, rows, width), BF), HBM)] * zn


GELU_ONE = 0.7978845608028654
GELU_TWO = 0.044715


def gelu_both(p):
    square = p * p
    th = jnp.tanh(GELU_ONE * (p + GELU_TWO * p * square))
    half = 0.5 * (1.0 + th)
    slope = half + 0.5 * p * (1.0 - th * th) * GELU_ONE * (1.0 + 3.0 * GELU_TWO * square)
    return p * half, slope


class RowSum:
    def __init__(self, me, sizes, img, txt, recvx, sumb, recvz, total, xs, xr, zs, zr):
        self.me, self.sizes, self.img, self.txt = me, sizes, img, txt
        self.recvx, self.sumb, self.recvz, self.total = recvx, sumb, recvz, total
        self.xs, self.xr, self.zs, self.zr = xs, xr, zs, zr
        self.sent, self.over_z = {}, []

    def send(self, s):
        me, (n_img, n_txt) = self.me, self.sizes
        zb = me.ahead(s)
        theirs = pl.ds(pl.multiple_of((zb * 2 + me.t_x) * n_img, n_img), n_img)
        where = {TP: me.t_x}
        self.sent[s] = [
            remote(
                self.img.at[theirs], self.recvx.at[s, pl.ds(0, n_img)], self.xs.at[s, 0], self.xr.at[s, 0], where
            ),
            remote(
                self.txt.at[zb, me.t_x],
                self.recvx.at[s, pl.ds(n_img, n_txt)],
                self.xs.at[s, 1],
                self.xr.at[s, 1],
                where,
            ),
        ]

    def add(self, s):
        me, (n_img, n_txt) = self.me, self.sizes
        zb = me.ahead(s)
        for copy in self.sent[s]:
            copy.wait()

        def put(to, value):
            if s:
                self.sumb[s, to] = value.astype(BF)
            else:
                self.total[to] = value

        @pl.loop(0, n_img // STEP)
        def _(i):
            to = pl.ds(pl.multiple_of(i * STEP, STEP), STEP)
            at = pl.ds(pl.multiple_of((zb * 2 + me.t) * n_img + i * STEP, STEP), STEP)
            put(to, self.img[at].astype(F32) + self.recvx[s, to].astype(F32))

        to = pl.ds(n_img, n_txt)
        put(to, self.txt[zb, me.t].astype(F32) + self.recvx[s, to].astype(F32))
        if s:
            self.over_z.append(
                remote(self.sumb.at[s], self.recvz.at[s], self.zs.at[s], self.zr.at[s], {CTX: zb})
            )

    def arrive(self):
        for copy in self.over_z:
            copy.wait()

    def rows(self, at):
        value = self.total[at]
        for s in range(1, self.me.zn):
            value = value + self.recvz[s, at].astype(F32)
        return value


def row_scratch(zn, sizes, dim):
    n_img, n_txt = sizes
    block = n_img + n_txt
    return [
        pltpu.VMEM((2 * zn * n_img, dim), BF),
        pltpu.VMEM((zn, 2, n_txt, dim), BF),
        pltpu.VMEM((zn, block, dim), BF),
        pltpu.VMEM((zn, block, dim), BF),
        pltpu.VMEM((zn, block, dim), BF),
        pltpu.VMEM((block, dim), F32),
        DMA((zn, 2)), DMA((zn, 2)), DMA((zn,)), DMA((zn,)),
    ]


ROW_SCRATCH = 10


def turn_kernel(zn, sizes, *refs):
    take = iter(refs)
    him, htx, cim, ctx, resid, proj, mod, gu, gd, ctx4 = [next(take) for _ in range(10)]
    bi, bt, out, rgrad, sums = [next(take) for _ in range(5)]
    pieces = [next(take) for _ in range(zn)]
    up, down, act, pre, branch, grads, cotr = [next(take) for _ in range(7)]
    h_refs = [next(take) for _ in range(ROW_SCRATCH)]
    m_refs = [next(take) for _ in range(ROW_SCRATCH)]
    bb, gzs, gzr, gxs, gxr, gloc = [next(take) for _ in range(6)]
    pair_refs = [next(take) for _ in range(8)]
    (loc,) = take
    me = Place(zn)
    n_img, n_txt = sizes
    img_all = 2 * zn * n_img
    h_sum, m_sum = RowSum(me, sizes, *h_refs), RowSum(me, sizes, *m_refs)
    pair = PairSum(me, grads, pieces, *pair_refs)
    load_up = local(gu, up, loc.at[0])
    load_down = local(gd, down, loc.at[1])
    mine = pl.ds(pl.multiple_of((me.c * 2 + me.t) * n_img, n_img), n_img)
    load_cot = [
        local(cim.at[mine], cotr.at[pl.ds(0, n_img)], loc.at[2]),
        local(ctx4.at[me.c, me.t], cotr.at[pl.ds(n_img, n_txt)], loc.at[3]),
    ]
    me.greet()
    load_up.wait()
    load_down.wait()

    def text_rows(ref, value):
        for zb in range(zn):
            for half in range(2):
                first = (zb * 2 + half) * n_txt
                ref[zb, half] = value[first : first + n_txt].astype(BF)

    def front_half(stream, hidden, cot, places):
        p = dot(hidden, up[stream], (1, 0))
        activated, slope = gelu_both(p)
        low = (cot.astype(F32) * line(mod, stream, 5)).astype(BF)
        grad = (dot(low, down[stream], (1, 0)) * slope).astype(BF)
        activated = activated.astype(BF)
        at = 0
        for place in places:
            n = place.size
            act[place] = activated[at : at + n]
            pre[place] = grad[at : at + n]
            branch[place] = low[at : at + n]
            at += n
        return dot(grad, up[stream], (1, 1))

    txt_place = pl.ds(img_all, 2 * zn * n_txt)
    text_rows(h_sum.txt, front_half(1, htx[...], ctx[...], [txt_place]))
    order = list(range(1, zn)) + [0]
    for first in range(0, zn, 2):
        steps = order[first : first + 2]
        places = [
            pl.ds(pl.multiple_of(me.ahead(s) * 2 * n_img, 2 * n_img), 2 * n_img) for s in steps
        ]
        value = front_half(
            0,
            jnp.concatenate([him[place] for place in places], axis=0),
            jnp.concatenate([cim[place] for place in places], axis=0),
            places,
        ).astype(BF)
        for n, (s, place) in enumerate(zip(steps, places)):
            h_sum.img[place] = value[n * 2 * n_img : (n + 1) * 2 * n_img]
            h_sum.send(s)
    text_rows(m_sum.txt, dot(act[txt_place], down[1], (1, 1)))
    for first in range(0, img_all, 256):
        rows = slice(first, first + 256)
        m_sum.img[rows] = dot(act[rows], down[0], (1, 1)).astype(BF)
    for s in order:
        m_sum.send(s)
    h_sum.add(order[0])
    parts = ((0, pl.ds(0, img_all)), (1, txt_place))
    dim = him.shape[1]

    def gradient(kind, at):
        stream, place = parts[at % 2]
        for first in range(0, dim, 256):
            d = slice(first, first + 256)
            if kind == 0:
                left = him[:, d] if stream == 0 else htx[:, d]
                value = dot(left, pre[place], (0, 0))
            else:
                value = dot(branch[place, d], act[place], (0, 0))
            grads[kind, stream, d] = value.astype(BF)
        pair.start(kind * 2 + stream)

    work = [lambda n=n: gradient(*divmod(n, 2)) for n in range(4)]
    for n, s in enumerate(order[1:]):
        work[n]()
        h_sum.add(s)
    work[3]()
    sums[...] = jnp.zeros_like(sums)
    pair.across(0)
    h_sum.arrive()
    for copy in load_cot:
        copy.wait()

    def rows(stream, at):
        h = h_sum.rows(at)
        normed, spread_ = layer_norm(resid[at])
        value = cotr[at].astype(F32) + norm_back(h * (1.0 + line(mod, stream, 4)), normed, spread_)
        rgrad[at] = value
        bb[at] = (value * line(mod, stream, 2)).astype(BF)
        sums[stream, 0] += jnp.sum(value * proj[at], axis=0)
        sums[stream, 1] += jnp.sum(h, axis=0)
        sums[stream, 2] += jnp.sum(h * normed, axis=0)

    row_loops(sizes, rows)
    shared = share_start(me, bb, (bi, bt), sizes, gzs, gzr, gxs, gxr, gloc)
    for s in order:
        m_sum.add(s)
    for n in range(1, 4):
        pair.across(n)
    share_end(me, shared, (bi, bt), gxs, gxr)
    m_sum.arrive()

    def last(stream, at):
        m = m_sum.rows(at)
        out[at] = (resid[at] + line(mod, stream, 5) * m).astype(BF)
        sums[stream, 3] += jnp.sum(cotr[at].astype(F32) * m, axis=0)

    row_loops(sizes, last)
    pair.end()


def turn(zn, sizes, him, htx, cim, ctx, resid, proj, mod, gu, gd):
    total, dim = resid.shape
    n_img, n_txt = sizes
    ff = gu.shape[2]
    rows = dim // (4 * zn)
    every = 2 * zn * total
    ctx4 = ctx.reshape(zn, 2, n_txt, dim)
    return call(
        functools.partial(turn_kernel, zn, sizes),
        2,
        [VMEM] * 7 + [HBM] * 3,
        [
            (shaped((zn, 2, n_img, dim), BF), HBM),
            (shaped((zn, 2, n_txt, dim), BF), HBM),
            (shaped((total, dim), BF), VMEM),
            (shaped((total, dim), F32), VMEM),
            (shaped((2, 4, dim), F32), VMEM),
        ]
        + pair_outs(2, zn, rows, ff),
        [
            pltpu.VMEM((2, dim, ff), BF),
            pltpu.VMEM((2, dim, ff), BF),
            pltpu.VMEM((every, ff), BF),
            pltpu.VMEM((every, ff), BF),
            pltpu.VMEM((every, dim), BF),
            pltpu.VMEM((2, 2, dim, ff), BF),
            pltpu.VMEM((total, dim), BF),
        ]
        + row_scratch(zn, sizes, dim)
        + row_scratch(zn, sizes, dim)
        + share_scratch(zn, total, dim)
        + pair_scratch(2, zn, rows, ff)
        + [DMA((4,))],
        (him, htx, cim, ctx, resid, proj, mod, gu, gd, ctx4),
    )


def finish_kernel(
    zn, sizes, ai, at_, x_rows, rgrad, out, sums, gains, mod, da, oi, ot, gsum, *rest
):
    me = Place(zn)
    pieces, rest = rest[:zn], rest[zn:]
    (
        own, recvx, sumb, recvz, total, sxs, sxr, sloc, szs, szr,
        ob, msum, mx, slots, xs, xr, zs, zr, fs, fr, loc, ms, mr,
    ) = rest[:23]
    pair = PairSum(me, da, pieces, *rest[23:])
    me.greet()
    c, t = me.c, me.t
    n_img, n_txt = sizes
    copies = sum_start(me, [(ai, at_)], own, recvx, sxs, sxr, sloc)
    for n in range(2):
        pair.start(n)

    def keep(stream, at):
        ob[0, at] = out[at]

    row_loops(sizes, keep)
    zc = sum_x(me, 0, copies, own, recvx, sumb, recvz, total, szs, szr)
    msum[...] = jnp.zeros_like(msum)
    for n in range(2):
        pair.across(n)
    sum_z(me, 0, zc, recvz, total)

    def rows(stream, at):
        h = total[0, at]
        normed, spread_ = layer_norm(x_rows[at].astype(F32))
        value = rgrad[at] + norm_back(h * (1.0 + line(mod, stream, 1)), normed, spread_)
        ob[1, at] = value.astype(BF)
        msum[stream * 6] += jnp.sum(h, axis=0)
        msum[stream * 6 + 1] += jnp.sum(h * normed, axis=0)

    row_loops(sizes, rows)
    for stream in range(2):
        for which in range(4):
            msum[stream * 6 + 2 + which] = sums[stream, which]
    msum[12] = gains[0]
    m_x = remote(msum, mx, ms.at[0], mr.at[0], {TP: me.t_x})
    img = ob.at[:, pl.ds(0, n_img)]
    txt = ob.at[:, pl.ds(n_img, n_txt)]
    done = [
        remote(img, oi.at[:, t], xs.at[0], xr.at[0], {TP: me.t_x}),
        remote(txt, ot.at[:, c, t], xs.at[1], xr.at[1], {TP: me.t_x}),
        local(img, oi.at[:, t], loc.at[0]),
        local(txt, ot.at[:, c, t], loc.at[1]),
    ]
    over_z = [
        remote(txt, ot.at[:, c, t], zs.at[s], zr.at[s], {CTX: me.ahead(s)}) for s in range(1, zn)
    ]
    m_x.wait()
    slots[c] = msum[...] + mx[...]
    m_z = [
        remote(slots.at[c], slots.at[c], ms.at[s], mr.at[s], {CTX: me.ahead(s)}) for s in range(1, zn)
    ]
    for s in range(1, zn):
        over_z[s - 1].wait()
        src = me.behind(s)
        done.append(
            remote(ot.at[:, src, t], ot.at[:, src, t], fs.at[s], fr.at[s], {TP: me.t_x})
        )
    for copy in m_z:
        copy.wait()
    value = slots[0]
    for z in range(1, zn):
        value = value + slots[z]
    gsum[me.d] = value
    m_c = remote(gsum.at[me.d], gsum.at[me.d], ms.at[zn], mr.at[zn], {DP: me.d_core})
    m_c.wait()
    both = gsum.at[pl.ds(me.y * 2, 2)]
    m_y = remote(both, both, ms.at[zn + 1], mr.at[zn + 1], {DP: me.d_y})
    pair.end()
    m_y.wait()
    for copy in done:
        copy.wait()


def finish(zn, sizes, ai, at_, x_rows, rgrad, out, sums, gains, mod, da):
    total, dim = rgrad.shape
    rows, width = dim // (4 * zn), da.shape[3]
    n_img, n_txt = sizes
    return call(
        functools.partial(finish_kernel, zn, sizes),
        3,
        [HBM] * 2 + [VMEM] * 7,
        [
            (shaped((2, 2, n_img, dim), BF), HBM),
            (shaped((2, zn, 2, n_txt, dim), BF), HBM),
            (shaped((4, 16, dim), F32), VMEM),
        ]
        + pair_outs(1, zn, rows, width),
        sum_scratch(1, zn, total, dim)
        + [
            pltpu.VMEM((2, total, dim), BF),
            pltpu.VMEM((16, dim), F32),
            pltpu.VMEM((16, dim), F32),
            pltpu.VMEM((zn, 16, dim), F32),
            DMA((2,)), DMA((2,)), DMA((zn,)), DMA((zn,)), DMA((zn,)), DMA((zn,)), DMA((2,)),
            DMA((zn + 2,)), DMA((zn + 2,)),
        ]
        + pair_scratch(1, zn, rows, width),
        (ai, at_, x_rows, rgrad, out, sums, gains, mod, da),
    )


def over_ctx(zn, pieces):
    return [pieces[0]] + [
        lax.ppermute(pieces[s], CTX, [(i, (i + s) % zn) for i in range(zn)]) for s in range(1, zn)
    ]


def own_call(kernel, ins, outs, scratch, args, flops, moved):
    return pl.pallas_call(
        kernel,
        out_shape=[shape for shape, _ in outs],
        in_specs=ins,
        out_specs=[spec for _, spec in outs],
        scratch_shapes=scratch,
        compiler_params=pltpu.CompilerParams(vmem_limit_bytes=60 * 1024 * 1024),
        cost_estimate=pl.CostEstimate(flops=flops, bytes_accessed=moved, transcendentals=0),
    )(*args)


def dot(one, two, dims):
    return lax.dot_general(one, two, ((dims[:1], dims[1:]), ((), ())), preferred_element_type=F32)


STEP = 16
EXP_MIN = -1e30


def blocks_of(sizes, largest):
    at = 0
    for stream, n in enumerate(sizes):
        size = largest if n % largest == 0 else n
        for i in range(n // size):
            yield stream, at + i * size, size
        at += n


def head_norms(packed, gains, stream, head, rows, heads):
    wide = gains.shape[-1]
    out = []
    for which in range(2):
        raw = packed[rows, (which * heads + head) * wide : (which * heads + head + 1) * wide]
        normed, factor = rms_norm(raw)
        out += [normed, factor]
    value = packed[rows, (2 * heads + head) * wide : (2 * heads + head + 1) * wide]
    return (*out, value)


def fill_heads(packed, gains, sizes, heads, q_s, k_s, v_s):
    for stream, first, size in blocks_of(sizes, 64):
        rows = slice(first, first + size)
        for head in range(heads):
            q, _, k, _, v = head_norms(packed, gains, stream, head, rows, heads)
            q_s[head, rows] = (q * gains[stream * 2][None, :]).astype(BF)
            k_s[head, rows] = (k * gains[stream * 2 + 1][None, :]).astype(BF)
            v_s[head, rows] = v.astype(BF)


def forward_kernel(zn, live, sizes, heads, *refs):
    take = iter(refs)
    cond, modw, qkv, out, txt, gains = [next(take) for _ in range(6)]
    up, down, xi, txt4, ci = [next(take) for _ in range(5)]
    hidden_o, packed_o, lse_o, att_o, ga_o, hi, ht, co, gu, gd = [next(take) for _ in range(10)]
    resid, proj, mod = [next(take) for _ in range(3)]
    (
        wa, mp, cbuf, pieces, ga, xo, xr, hidden, packed, lse, attended, q_s, k_s, v_s, flat, pim, ptx,
        my, m2, mc, m1, mx, slots, recvx, sumb, recvz, total, hb, bx,
        tzs, tzr, txs, txr, azs, azr, ays, ayr, acs, acr, ms, mr,
        uzs, uzr, uys, uyr, ucs, ucr, sxs, sxr, szs, szr, gzs, gzr, gxs, gxr, gloc,
        czs, czr, cxs, cxr, loc, uloc,
    ) = take
    me = Place(zn)
    d, c, t, y, k = me.d, me.c, me.t, me.y, me.k
    n_img, n_txt = sizes
    img_all, txt_all = 2 * zn * n_img, 2 * zn * n_txt
    rows_w, width = wa.shape[2:]
    wide = gains.shape[-1]
    col = heads * wide
    ahead = list(range(1, zn))

    ff = up.shape[2] // zn
    cuts = {}
    for s in ahead + [0]:
        cols = pl.ds(pl.multiple_of(me.ahead(s) * ff, ff), ff)
        for kind, w in enumerate((up, down)):
            cuts[s, kind] = local(w.at[:, :, cols], cbuf.at[s, kind], uloc.at[s, kind])
    row_of = [(c * 2 + half) * n_img for half in range(2)]
    loads = [
        local(xi.at[half], xo.at[pl.ds(pl.multiple_of(row_of[half], n_img), n_img)], loc.at[half])
        for half in range(2)
    ]
    loads.append(local(xi.at[t], xr.at[pl.ds(0, n_img)], loc.at[2]))
    loads.append(local(txt4.at[c, t], xr.at[pl.ds(n_img, n_txt)], loc.at[3]))
    load_c = local(ci, bx, loc.at[4])

    me.greet()
    mine = pl.ds(pl.multiple_of((c * 2 + t) * n_img, n_img), n_img)
    tokens = [
        remote(xi.at[t], xo.at[mine], tzs.at[s], tzr.at[s], {CTX: me.ahead(s)}) for s in ahead
    ]
    value = cond[...].astype(F32)
    act = (value / (1.0 + jnp.exp(-value))).astype(BF)
    for st in range(2):
        for which in range(6):
            part = dot(act, modw[st, which].astype(BF), (1, 0))
            for seq in range(part.shape[0]):
                mp[seq, st * 6 + which] = part[seq]
    m_y = remote(mp.at[pl.ds((1 - y) * 2, 2)], my, ms.at[0], mr.at[0], {DP: me.d_y})
    weights = []
    block = pl.ds(pl.multiple_of((d * zn + c) * rows_w, rows_w), rows_w)
    for st in range(2):
        for kind in range(4):
            whole = (qkv[st, kind] if kind < 3 else out[st]).astype(BF)
            for z in range(zn):
                wa[z, st, :, kind * col : (kind + 1) * col] = whole[:, z * col : (z + 1) * col]
        weights.append(
            [
                remote(
                    wa.at[me.ahead(s), st], ga.at[st, block], azs.at[st, s], azr.at[st, s],
                    {CTX: me.ahead(s)},
                )
                for s in ahead
            ]
        )
    own_a = [local(wa.at[c, st], ga.at[st, block], loc.at[5 + st]) for st in range(2)]
    m_y.wait()
    m2[...] = mp[pl.ds(y * 2, 2)] + my[...]
    m_c = remote(m2.at[1 - k], mc, ms.at[1], mr.at[1], {DP: me.d_core})
    m_c.wait()
    m1[...] = m2[k] + mc[...]
    m_x = remote(m1, mx, ms.at[2], mr.at[2], {TP: me.t_x})
    for s in ahead + [0]:
        for kind in range(2):
            cuts[s, kind].wait()
            for st in range(2):
                pieces[s, kind, st] = cbuf[s, kind, st].astype(BF)
    m_x.wait()
    slots[c] = m1[...] + mx[...]
    m_z = [
        remote(slots.at[c], slots.at[c], ms.at[2 + s], mr.at[2 + s], {CTX: me.ahead(s)})
        for s in ahead
    ]
    outs = (gu, gd)
    pairs = [(kind, st) for kind in range(2) for st in range(2)]
    mlp, own_u = {}, {}
    for n, (kind, st) in enumerate(pairs):
        dst = outs[kind].at[st, d * zn + c]
        mlp[n] = [
            remote(pieces.at[s, kind, st], dst, uzs.at[n, s], uzr.at[n, s], {CTX: me.ahead(s)})
            for s in ahead
        ]
        own_u[n] = local(pieces.at[0, kind, st], dst, loc.at[7 + n])
    pending = []
    over_y = []
    rows_y = [
        pl.ds(pl.multiple_of(dd * zn * rows_w, zn * rows_w), zn * rows_w) for dd in (d, me.d_y)
    ]
    for st in range(2):
        for copy in weights[st]:
            copy.wait()
        own_a[st].wait()
        here = ga.at[st, rows_y[0]]
        over_y.append(remote(here, here, ays.at[st], ayr.at[st], {DP: me.d_y}))
        pending.append(remote(here, here, acs.at[st, 0], acr.at[st, 0], {DP: me.d_core}))
    for s in ahead:
        tokens[s - 1].wait()
        here = xo.at[pl.ds(pl.multiple_of((me.behind(s) * 2 + t) * n_img, n_img), n_img)]
        pending.append(remote(here, here, txs.at[s], txr.at[s], {TP: me.t_x}))
    for st in range(2):
        over_y[st].wait()
        there = ga.at[st, rows_y[1]]
        pending.append(remote(there, there, acs.at[st, 1], acr.at[st, 1], {DP: me.d_core}))
    for copy in m_z:
        copy.wait()
    value = slots[0]
    for z in range(1, zn):
        value = value + slots[z]
    mod[...] = value
    for copy in loads + pending:
        copy.wait()
    saves = [local(ga, ga_o, loc.at[11])]

    at = 0
    for stream, (rows_in, n) in enumerate(((xo, img_all), (txt, txt_all))):

        @pl.loop(0, n // STEP)
        def _(i, rows_in=rows_in, stream=stream, at=at):
            here = pl.ds(pl.multiple_of(i * STEP, STEP), STEP)
            normed, _ = layer_norm(rows_in[here].astype(F32))
            value = normed * (1.0 + line(mod, stream, 1)) + line(mod, stream, 0)
            hidden[pl.ds(pl.multiple_of(at + i * STEP, STEP), STEP)] = value.astype(BF)

        at += n
    streams = (img_all, txt_all)
    for stream, first, size in blocks_of(streams, 256):
        rows = slice(first, first + size)
        packed[rows] = dot(hidden[rows], ga[stream, :, : 3 * col], (1, 0))
    saves.append(local(hidden, hidden_o, loc.at[12]))
    saves.append(local(packed, packed_o, loc.at[13]))
    fill_heads(packed, gains, streams, heads, q_s, k_s, v_s)
    flat[...] = jnp.zeros_like(flat)
    size = (img_all + txt_all) // 4
    scale = wide ** (-0.5)
    lanes = flat.shape[1]
    for head in range(heads):

        @pl.loop(0, 4)
        def _(i, head=head):
            rows = pl.ds(pl.multiple_of(i * size, STEP), size)
            scores = dot(q_s[head, rows], k_s[head], (1, 1)) * scale
            index = lax.broadcasted_iota(jnp.int32, scores.shape, 1)
            scores = jnp.where(index < live, scores, EXP_MIN)
            peak = jnp.max(scores, axis=-1, keepdims=True)
            log_total = peak + jnp.log(jnp.sum(jnp.exp(scores - peak), axis=-1, keepdims=True))
            probs = jnp.exp(scores - log_total).astype(BF)
            lse[rows, head : head + 1] = log_total
            value = dot(probs, v_s[head], (1, 0))
            attended[rows, head * wide : (head + 1) * wide] = value
            lane = lanes - (heads - head) * wide
            flat[rows, lane : lane + wide] = value.astype(BF)

    saves.append(local(lse, lse_o, loc.at[14]))
    saves.append(local(attended, att_o, loc.at[15]))

    sent = {}
    for s in ahead + [0]:
        zb = me.ahead(s)
        rows = pl.ds(pl.multiple_of(zb * 2 * n_img, 2 * n_img), 2 * n_img)
        pim[rows] = dot(flat[rows], ga[0, :, width - lanes :], (1, 1)).astype(BF)
        rows = pl.ds(pl.multiple_of(img_all + zb * 2 * n_txt, STEP), 2 * n_txt)
        part = dot(flat[rows], ga[1, :, width - lanes :], (1, 1))
        for half in range(2):
            ptx[zb, half] = part[half * n_txt : (half + 1) * n_txt].astype(BF)
        theirs = pl.ds(pl.multiple_of((zb * 2 + me.t_x) * n_img, n_img), n_img)
        sent[s] = [
            remote(pim.at[theirs], recvx.at[s, pl.ds(0, n_img)], sxs.at[s, 0], sxr.at[s, 0], {TP: me.t_x}),
            remote(ptx.at[zb, me.t_x], recvx.at[s, pl.ds(n_img, n_txt)], sxs.at[s, 1], sxr.at[s, 1], {TP: me.t_x}),
        ]
    u_y, u_pending = [], []

    def weights_on(n):
        kind, st = pairs[n]
        for copy in mlp[n]:
            copy.wait()
        own_u[n].wait()
        here = outs[kind].at[st, pl.ds(d * zn, zn)]
        u_y.append(remote(here, here, uys.at[n], uyr.at[n], {DP: me.d_y}))
        u_pending.append(remote(here, here, ucs.at[n, 0], ucr.at[n, 0], {DP: me.d_core}))

    def weights_last(n):
        kind, st = pairs[n]
        u_y[n].wait()
        there = outs[kind].at[st, pl.ds(me.d_y * zn, zn)]
        u_pending.append(remote(there, there, ucs.at[n, 1], ucr.at[n, 1], {DP: me.d_core}))

    zc = []
    for s in ahead + [0]:
        zb = me.ahead(s)
        for copy in sent[s]:
            copy.wait()

        def put(to, value, s=s):
            if s:
                sumb[s, to] = value.astype(BF)
            else:
                total[to] = value

        @pl.loop(0, n_img // STEP)
        def _(i, s=s, zb=zb, put=put):
            to = pl.ds(pl.multiple_of(i * STEP, STEP), STEP)
            at = pl.ds(pl.multiple_of((zb * 2 + t) * n_img + i * STEP, STEP), STEP)
            put(to, pim[at].astype(F32) + recvx[s, to].astype(F32))

        to = pl.ds(n_img, n_txt)
        put(to, ptx[zb, t].astype(F32) + recvx[s, to].astype(F32))
        if s:
            zc.append(remote(sumb.at[s], recvz.at[s], szs.at[s], szr.at[s], {CTX: zb}))
        weights_on(ahead.index(s) if s else zn - 1)
    for n in range(zn, 4):
        weights_on(n)
    for copy in zc:
        copy.wait()

    def rows(stream, at):
        p = total[at]
        for s in ahead:
            p = p + recvz[s, at].astype(F32)
        proj[at] = p
        value = xr[at].astype(F32) + line(mod, stream, 2) * p
        resid[at] = value
        normed, _ = layer_norm(value)
        hb[at] = (normed * (1.0 + line(mod, stream, 4)) + line(mod, stream, 3)).astype(BF)

    row_loops(sizes, rows)
    shared = share_start(me, hb, (hi, ht), sizes, gzs, gzr, gxs, gxr, gloc)
    cots = [
        remote(ci.at[t], co.at[c, t], czs.at[s], czr.at[s], {CTX: me.ahead(s)}) for s in ahead
    ]
    load_c.wait()
    saves.append(local(bx, co.at[c], loc.at[16]))
    for n in range(4):
        weights_last(n)
    share_end(me, shared, (hi, ht), gxs, gxr)
    for s in ahead:
        cots[s - 1].wait()
        here = co.at[me.behind(s), t]
        u_pending.append(remote(here, here, cxs.at[s], cxr.at[s], {TP: me.t_x}))
    for copy in u_pending + saves:
        copy.wait()


def forward(zn, live, sizes, heads, cond, modw, qkv, out, txt, gains, up, down, xi, ci):
    n_img, n_txt = sizes
    dim = txt.shape[1]
    rows, wide_out = out.shape[1:]
    ff = up.shape[2] // zn
    wide = gains.shape[-1]
    col = heads * wide
    width = 4 * col
    total, block = 2 * zn * (n_img + n_txt), n_img + n_txt
    lanes = -(-col // 128) * 128
    seqs = cond.shape[0]
    txt4 = txt.reshape(zn, 2, n_txt, dim)
    weight = (shaped((2, 4 * zn, rows, ff), BF), HBM)
    return call(
        functools.partial(forward_kernel, zn, live, sizes, heads),
        0,
        [VMEM] * 6 + [HBM] * 5,
        [
            (shaped((total, dim), BF), HBM),
            (shaped((total, 3 * col), F32), HBM),
            (shaped((total, 128), F32), HBM),
            (shaped((total, col), F32), HBM),
            (shaped((2, dim, width), BF), HBM),
            (shaped((zn, 2, n_img, dim), BF), HBM),
            (shaped((zn, 2, n_txt, dim), BF), HBM),
            (shaped((zn, 2, n_img, dim), BF), HBM),
            weight,
            weight,
            (shaped((block, dim), F32), VMEM),
            (shaped((block, dim), F32), VMEM),
            (shaped((12, dim), F32), VMEM),
        ],
        [
            pltpu.VMEM((zn, 2, rows, width), BF),
            pltpu.VMEM((seqs, 12, dim), F32),
            pltpu.VMEM((zn, 2, 2, rows, ff), F32),
            pltpu.VMEM((zn, 2, 2, rows, ff), BF),
            pltpu.VMEM((2, dim, width), BF),
            pltpu.VMEM((2 * zn * n_img, dim), BF),
            pltpu.VMEM((block, dim), BF),
            pltpu.VMEM((total, dim), BF),
            pltpu.VMEM((total, 3 * col), F32),
            pltpu.VMEM((total, 128), F32),
            pltpu.VMEM((total, col), F32),
            pltpu.VMEM((heads, total, wide), BF),
            pltpu.VMEM((heads, total, wide), BF),
            pltpu.VMEM((heads, total, wide), BF),
            pltpu.VMEM((total, lanes), BF),
            pltpu.VMEM((2 * zn * n_img, dim), BF),
            pltpu.VMEM((zn, 2, n_txt, dim), BF),
            pltpu.VMEM((2, 12, dim), F32),
            pltpu.VMEM((2, 12, dim), F32),
            pltpu.VMEM((12, dim), F32),
            pltpu.VMEM((12, dim), F32),
            pltpu.VMEM((12, dim), F32),
            pltpu.VMEM((zn, 12, dim), F32),
            pltpu.VMEM((zn, block, dim), BF),
            pltpu.VMEM((zn, block, dim), BF),
            pltpu.VMEM((zn, block, dim), BF),
            pltpu.VMEM((block, dim), F32),
            pltpu.VMEM((block, dim), BF),
            pltpu.VMEM((2, n_img, dim), BF),
            DMA((zn,)), DMA((zn,)), DMA((zn,)), DMA((zn,)),
            DMA((2, zn)), DMA((2, zn)), DMA((2,)), DMA((2,)), DMA((2, 2)), DMA((2, 2)),
            DMA((2 + zn,)), DMA((2 + zn,)),
            DMA((4, zn)), DMA((4, zn)), DMA((4,)), DMA((4,)), DMA((4, 2)), DMA((4, 2)),
            DMA((zn, 2)), DMA((zn, 2)), DMA((zn,)), DMA((zn,)),
            DMA((2, zn)), DMA((2, zn)), DMA((2, zn)), DMA((2, zn)), DMA((2,)),
            DMA((zn,)), DMA((zn,)), DMA((zn,)), DMA((zn,)),
            DMA((17,)), DMA((zn, 2)),
        ],
        (cond, modw, qkv, out, txt, gains, up, down, xi, txt4, ci),
    )


def back_kernel(
    live, sizes, heads, bi, bt, ga, hidden, packed, lse, attended, gains, ai, at_, da, gain_row,
    q_s, k_s, v_s, g_s, flat, stat, dq, dk, dv, pg,
):
    wide = gains.shape[-1]
    scale = wide ** (-0.5)
    total = sum(sizes)
    lanes = flat.shape[1]
    fill_heads(packed, gains, sizes, heads, q_s, k_s, v_s)
    flat[...] = jnp.zeros_like(flat)
    stat[...] = jnp.zeros_like(stat)
    stat[:total] = lse[...]
    pg[...] = jnp.zeros_like(pg)
    first_lane = lanes - heads * wide

    def branch(stream, first, size):
        ref = bi if stream == 0 else bt
        base = first if stream == 0 else first - sizes[0]
        return ref[base : base + size]

    flat[:, first_lane:] = attended[...].astype(BF)
    for stream, first, size in blocks_of(sizes, 256):
        rows = slice(first, first + size)
        grad = dot(branch(stream, first, size), ga[stream, :, ga.shape[2] - lanes :], (1, 0)).astype(BF)
        for head in range(heads):
            part = grad[:, first_lane + head * wide : first_lane + (head + 1) * wide]
            g_s[head, rows] = part
            value = attended[rows, head * wide : (head + 1) * wide]
            stat[rows, heads + head : heads + head + 1] = jnp.sum(
                part.astype(F32) * value, axis=-1, keepdims=True
            )
    across = jnp.transpose(stat[...])
    size = total // 4
    for head in range(heads):
        lse_row = across[head : head + 1, :total]
        delta_row = across[heads + head : heads + head + 1, :total]
        for i in range(4):
            rows = slice(i * size, (i + 1) * size)
            scores = dot(k_s[head, rows], q_s[head], (1, 1)) * scale
            probs = jnp.exp(scores - lse_row)
            if (i + 1) * size > live:
                index = lax.broadcasted_iota(jnp.int32, scores.shape, 0) + i * size
                probs = jnp.where(index < live, probs, 0.0)
            prob_grad = dot(v_s[head, rows], g_s[head], (1, 1))
            score_grad = (probs * (prob_grad - delta_row) * scale).astype(BF)
            dk[head, rows] = dot(score_grad, q_s[head], (1, 0))
            dv[head, rows] = dot(probs.astype(BF), g_s[head], (1, 0))
            part = dot(score_grad, k_s[head, rows], (0, 0))
            dq[head] = part if i == 0 else dq[head] + part
    sums = [[jnp.zeros((1, wide), F32) for _ in range(2)] for _ in range(2)]
    for stream, first, size in blocks_of(sizes, 64):
        rows = slice(first, first + size)
        for head in range(heads):
            q, q_factor, k, k_factor, _ = head_norms(packed, gains, stream, head, rows, heads)
            for which, (normed, factor, grad) in enumerate(
                ((q, q_factor, dq[head, rows]), (k, k_factor, dk[head, rows]))
            ):
                sums[stream][which] += jnp.sum(grad * normed, axis=0, keepdims=True)
                raw = rms_back(grad * gains[stream * 2 + which][None, :], normed, factor)
                lane = (which * heads + head) * wide
                pg[rows, lane : lane + wide] = raw.astype(BF)
            lane = (2 * heads + head) * wide
            pg[rows, lane : lane + wide] = dv[head, rows].astype(BF)
    gain_row[...] = jnp.zeros_like(gain_row)
    for stream in range(2):
        for which in range(2):
            lane = (stream * 2 + which) * wide
            gain_row[:, lane : lane + wide] = sums[stream][which]
    width = 3 * heads * wide
    for stream, first, size in blocks_of(sizes, 256):
        out = ai if stream == 0 else at_
        base = first if stream == 0 else first - sizes[0]
        out[base : base + size] = dot(
            pg[first : first + size, :width], ga[stream, :, :width], (1, 1)
        ).astype(BF)
    dim = hidden.shape[1]
    cut_at = ga.shape[2] - lanes
    cols = dim // 6
    at = 0
    for stream, n in enumerate(sizes):
        rows = slice(at, at + n)
        for j in range(6):
            d = slice(j * cols, (j + 1) * cols)
            one = dot(hidden[rows, d], pg[rows], (0, 0))
            ref = bi if stream == 0 else bt
            two = dot(ref[:, d], flat[rows], (0, 0))
            da[stream, d, :cut_at] = one[:, :cut_at].astype(BF)
            over = pg.shape[1] - cut_at
            da[stream, d, cut_at : cut_at + over] = (one[:, cut_at:] + two[:, :over]).astype(BF)
            da[stream, d, cut_at + over :] = two[:, over:].astype(BF)
        at += n


def back(live, sizes, heads, bi, bt, ga, hidden, packed, lse, attended, gains):
    total, dim = hidden.shape
    wide = gains.shape[-1]
    lanes = -(-heads * wide // 128) * 128
    stat_rows = -(-total // 128) * 128
    return own_call(
        functools.partial(back_kernel, live, sizes, heads),
        [VMEM] * 8,
        [
            (shaped(bi.shape, BF), VMEM),
            (shaped(bt.shape, BF), VMEM),
            (shaped(ga.shape, BF), VMEM),
            (shaped((1, dim), F32), VMEM),
        ],
        [pltpu.VMEM((heads, total, wide), BF)] * 4
        + [pltpu.VMEM((total, lanes), BF), pltpu.VMEM((stat_rows, 128), F32)]
        + [pltpu.VMEM((heads, total, wide), F32)] * 3
        + [pltpu.VMEM((total, -(-3 * heads * wide // 128) * 128), BF)],
        (bi, bt, ga, hidden, packed, lse, attended, gains),
        8 * 10**9,
        4 * 10**7,
    )


def adam_parts(weight, moment, second, gradient):
    new_moment = beta_one * moment + (1.0 - beta_one) * gradient
    new_second = beta_two * second + (1.0 - beta_two) * gradient * gradient
    update = (new_moment * (1.0 / corr_one)) / (
        jnp.sqrt(new_second * (1.0 / corr_two)) + adam_eps
    ) + decay_rate * weight
    return weight - learn_rate * update, new_moment, new_second


def adam_rows(ins, outs, n, grad_of, rows):
    @pl.loop(0, rows // 32)
    def _(i):
        at = pl.ds(pl.multiple_of(i * 32, 32), 32)
        grad = grad_of(at)
        outs[0, n, at] = grad
        for j, part in enumerate(adam_parts(ins[0, n, at], ins[1, n, at], ins[2, n, at], grad)):
            outs[1 + j, n, at] = part


def mlp_adam_kernel(zn, *refs):
    me = Place(zn)
    take = iter(refs)
    mlp = [next(take) for _ in range(zn)]
    weights = [[next(take) for _ in range(3)] for _ in range(2)]
    results = [[next(take) for _ in range(4)] for _ in range(2)]
    pbuf, ins, outs, psem, isem, osem = take
    rows, width = pbuf.shape[3:]
    loads = [local(mlp[s], pbuf.at[s], psem.at[s]) for s in range(zn)]
    chunks = [(kind, st, src) for kind in range(2) for st in range(2) for src in range(zn)]
    copies = {}
    for n, (kind, st, src) in enumerate(chunks):
        cols = pl.ds(src * width, width)
        copies[n] = [
            local(weights[kind][i].at[st, :, cols], ins.at[i, n], isem.at[i, n]) for i in range(3)
        ]
    for copy in loads:
        copy.wait()
    last = []
    for n, (kind, st, src) in enumerate(chunks):
        piece = me.behind(src)
        cols = pl.ds(src * width, width)
        for copy in copies[n]:
            copy.wait()
        adam_rows(ins, outs, n, lambda at: pbuf[piece, kind, st, at].astype(F32), rows)
        last.extend(
            local(outs.at[j, n], results[kind][j].at[st, :, cols], osem.at[j, n]) for j in range(4)
        )
    for copy in last:
        copy.wait()


def mlp_adam(zn, pieces, up, down):
    rows, width = pieces[0].shape[2:]
    n = 4 * zn
    return own_call(
        functools.partial(mlp_adam_kernel, zn),
        [HBM] * (zn + 6),
        [(shaped(up[0].shape, F32), HBM)] * 8,
        [
            pltpu.VMEM((zn, 2, 2, rows, width), BF),
            pltpu.VMEM((3, n, rows, width), F32),
            pltpu.VMEM((4, n, rows, width), F32),
            DMA((zn,)), DMA((3, n)), DMA((4, n)),
        ],
        (*pieces, *up, *down),
        10**8,
        36 * 10**6,
    )


def att_adam_kernel(zn, *refs):
    me = Place(zn)
    take = iter(refs)
    pieces = [next(take) for _ in range(zn)]
    qkv, out = [next(take) for _ in range(3)], [next(take) for _ in range(3)]
    qkv_new, out_new = [next(take) for _ in range(4)], [next(take) for _ in range(4)]
    pbuf, grad, ins, outs, psem, isem, osem = take
    rows, wide = grad.shape[1:]
    col = wide // zn
    loads = [local(pieces[s].at[0], pbuf.at[s], psem.at[s]) for s in range(zn)]
    chunks = [(st, kind) for st in range(2) for kind in range(4)]

    def place(three, three_out, st, kind):
        return three.at[st, kind] if kind < 3 else three_out.at[st]

    copies = {}
    for n, (st, kind) in enumerate(chunks):
        copies[n] = [
            local(place(qkv[i], out[i], st, kind), ins.at[i, n], isem.at[i, n]) for i in range(3)
        ]
    for copy in loads:
        copy.wait()
    for n, (st, kind) in enumerate(chunks):
        for src in range(zn):
            piece = pbuf[me.behind(src), st, :, kind * col : (kind + 1) * col]
            grad[n, :, src * col : (src + 1) * col] = piece.astype(F32)
    last = []
    for n, (st, kind) in enumerate(chunks):
        for copy in copies[n]:
            copy.wait()
        adam_rows(ins, outs, n, lambda at: grad[n, at], rows)
        last.extend(
            local(outs.at[j, n], place(qkv_new[j], out_new[j], st, kind), osem.at[j, n])
            for j in range(4)
        )
    for copy in last:
        copy.wait()


def att_adam(zn, pieces, qkv, out):
    rows, width = pieces[0].shape[2:]
    wide = out[0].shape[2]
    return own_call(
        functools.partial(att_adam_kernel, zn),
        [HBM] * (zn + 6),
        [(shaped(qkv[0].shape, F32), HBM)] * 4 + [(shaped(out[0].shape, F32), HBM)] * 4,
        [
            pltpu.VMEM((zn, 2, rows, width), BF),
            pltpu.VMEM((8, rows, wide), F32),
            pltpu.VMEM((3, 8, rows, wide), F32),
            pltpu.VMEM((4, 8, rows, wide), F32),
            DMA((zn,)), DMA((3, 8)), DMA((4, 8)),
        ],
        (*pieces, *qkv, *out),
        10**8,
        18 * 10**6,
    )


def mod_adam_kernel(cond, sums, w, m, v, grad_out, w_out, m_out, v_out):
    value = cond[...].astype(F32)
    act = (value / (1.0 + jnp.exp(-value))).astype(BF).astype(F32)
    rows = w.shape[2]
    which = pl.program_id(0)
    for first in range(0, rows, 16):
        at = slice(first, first + 16)
        grad = act[at, 0:1] * sums[0, which][None, :]
        for seq in range(1, sums.shape[0]):
            grad = grad + act[at, seq : seq + 1] * sums[seq, which][None, :]
        grad_out[0, 0, at] = grad
        for ref, part in zip((w_out, m_out, v_out), adam_parts(w[0, 0, at], m[0, 0, at], v[0, 0, at], grad)):
            ref[0, 0, at] = part


def mod_adam(cond_cols, sums, three):
    rows, dim = three[0].shape[2:]
    spec = pl.BlockSpec((1, 1, rows, dim), lambda i: (i // 6, i % 6, 0, 0))
    return pl.pallas_call(
        mod_adam_kernel,
        out_shape=[shaped(three[0].shape, F32)] * 4,
        grid=(12,),
        in_specs=[
            pl.BlockSpec(cond_cols.shape, lambda i: (0, 0)),
            pl.BlockSpec(sums.shape, lambda i: (0, 0, 0)),
        ]
        + [spec] * 3,
        out_specs=[spec] * 4,
        cost_estimate=pl.CostEstimate(flops=10**7, bytes_accessed=25 * 10**6, transcendentals=0),
    )(cond_cols, sums, *three)


def split_body(
    img_in, txt_in, cond, mod_weight, qkv_weight, out_weight, up_weight, down_weight, norm_gain,
    cot_img, cot_txt, mod_moment, qkv_moment, out_moment, up_moment, down_moment, gain_moment,
    mod_second, qkv_second, out_second, up_second, down_second, gain_second,
):
    zn = lax.axis_size(CTX)
    dim = img_in.shape[2]
    img_dev, txt_len = img_in.shape[1], txt_in.shape[1]
    n_img = img_dev // 2
    n_txt = -(-txt_len // (2 * zn * CHUNK)) * CHUNK
    sizes = (n_img, n_txt)
    txt_pad = n_txt * 2 * zn
    img_all = img_dev * zn
    head_dim = norm_gain.shape[-1]
    rows = qkv_weight.shape[2]
    col = qkv_weight.shape[4] // zn
    heads = col // head_dim
    ff = up_weight.shape[3] // zn
    scale_factor = head_dim ** (-0.5)
    c, t = lax.axis_index(CTX), lax.axis_index(TP)
    seq = lax.axis_index(DP)
    n_seq = lax.axis_size(DP)

    def by_rows(four):
        return jnp.swapaxes(four[0], 1, 2)

    up_three = [value[0] for value in (up_weight, up_moment, up_second)]
    down_three = [by_rows(value) for value in (down_weight, down_moment, down_second)]
    out_three = [by_rows(value) for value in (out_weight, out_moment, out_second)]
    qkv_three = [by_rows(value) for value in (qkv_weight, qkv_moment, qkv_second)]
    mod_three = [by_rows(value) for value in (mod_weight, mod_moment, mod_second)]
    cot_rows_txt = jnp.pad(cot_txt[0], ((0, txt_pad - txt_len), (0, 0)))
    txt_rows = jnp.pad(txt_in[0], ((0, txt_pad - txt_len), (0, 0)))
    gains = norm_gain[0].reshape(4, head_dim)
    streams = (img_all, txt_pad)
    live = img_all + txt_len
    hidden, packed, lse, attended, ga, hi, ht, co, gu, gd, resid, proj_rows, mod = forward(
        zn, live, sizes, heads, cond, mod_three[0], qkv_three[0], out_three[0], txt_rows, gains,
        up_three[0], down_three[0], img_in.reshape(2, n_img, dim), cot_img.reshape(2, n_img, dim),
    )
    gu = gu.reshape(2, -1, ff)
    gd = gd.reshape(2, -1, ff)
    def own_rows(img, txt):
        one = lax.dynamic_slice_in_dim(img, t * n_img, n_img, 0)
        two = lax.dynamic_slice_in_dim(txt, (c * 2 + t) * n_txt, n_txt, 0)
        return jnp.concatenate([one, two], axis=0)

    x_rows = own_rows(img_in[0], txt_rows)
    def blocks(img, txt):
        return img.reshape(zn, 2, n_img, dim), txt.reshape(zn, 2, n_txt, dim)

    bi, bt, out_rows, rgrad, sums, *mlp_back = turn(
        zn, sizes, hi.reshape(img_all, dim), ht.reshape(txt_pad, dim), co.reshape(img_all, dim),
        cot_rows_txt, resid, proj_rows, mod, gu, gd,
    )
    mlp_grads = over_ctx(zn, mlp_back)

    *input_part, da, gain_row = back(
        live, streams, heads, bi.reshape(img_all, dim), bt.reshape(txt_pad, dim),
        ga, hidden, packed, lse, attended, gains,
    )
    oi, ot, gsum, *att_back = finish(
        zn, sizes, *blocks(*input_part), x_rows, rgrad, out_rows, sums, gain_row, mod,
        da[None],
    )
    mlp_new = mlp_adam(zn, mlp_grads, up_three, down_three)
    att_new = att_adam(zn, over_ctx(zn, att_back), qkv_three, out_three)
    mod_new = mod_adam(cond.T, gsum[:, :12], mod_three)
    img_out, img_grad = oi[0].reshape(1, img_dev, dim), oi[1].reshape(1, img_dev, dim)
    txt_out = ot[0].reshape(1, txt_pad, dim)[:, :txt_len]
    txt_grad = ot[1].reshape(1, txt_pad, dim)[:, :txt_len]

    gain_grad = jnp.sum(gsum[:, 12, : 4 * head_dim], axis=0).reshape(norm_gain.shape)

    def back_rows(value):
        return jnp.swapaxes(value, 1, 2)[None]

    results = [img_out, txt_out, img_grad, txt_grad]
    results += [back_rows(value) for value in mod_new + att_new]
    results += [value[None] for value in mlp_new[:4]]
    results += [back_rows(value) for value in mlp_new[4:]]
    results.append(gain_grad)
    results.extend(adam_step(norm_gain, gain_moment, gain_second, gain_grad))
    return tuple(results)


def fits_split(mesh, args):
    dp, zn, tp = (mesh.shape[axis] for axis in ALL)
    img, txt, gain, qkv, up = args[0], args[1], args[8], args[4], args[6]
    heads = qkv.shape[4] // gain.shape[-1]
    return (
        dp == 4
        and tp == 2
        and zn == 4
        and qkv.shape[0] == 1
        and img.shape[0] == dp
        and heads % (tp * zn) == 0
        and (4 * qkv.shape[4] // (tp * zn)) % 128 == 0
        and (up.shape[3] // (tp * zn)) % 128 == 0
        and img.shape[1] % (zn * 2 * CHUNK) == 0
        and img.shape[2] % 128 == 0
        and img.shape[2] % (dp * zn * CHUNK) == 0
        and 4 * gain.shape[-1] <= img.shape[2]
    )


def solution(mesh):
    tokens = [P(DP, CTX, None), P(DP, None, None)]
    mod_spec = P(None, None, ALL, None, None)
    qkv_spec = P(None, None, ROWS, None, TP)
    out_spec = P(None, None, TP, ROWS)
    up_spec = P(None, None, ROWS, TP)
    weights = [mod_spec, qkv_spec, out_spec, up_spec, out_spec, P()]
    in_specs = tuple(tokens + [P(None, ALL)] + weights + tokens + weights + weights)
    out_specs = tuple(tokens + tokens + [spec for spec in weights for _ in range(4)])

    def step(*args):
        body = split_body if fits_split(mesh, args) else gathered_body
        return jax.shard_map(
            body, mesh=mesh, in_specs=in_specs, out_specs=out_specs, check_vma=False
        )(*args)

    return step
```
